128 devices in a mesh: seq: 16 (over y, x), kvh: 8 (over z, core).
Axes of the slice: x: 4, y: 4, z: 4, core: 2. Of those that a mesh axis runs over, the one named last changes fastest.
Arguments:
- queries: bfloat16 [64, 64, 128], P(None, 'kvh'), may hold values from -128 to 128
- keys: bfloat16 [2048, 8, 128, 128], P('seq', 'kvh'), may hold values from -6 to 6
- values: bfloat16 [2048, 8, 128, 128], P('seq', 'kvh'), may hold values from -6 to 6
- rep_keys: bfloat16 [2048, 8, 4, 128], P('seq', 'kvh'), may hold values from -8 to 8
- rep_values: bfloat16 [2048, 8, 4, 128], P('seq', 'kvh'), may hold values from -6 to 6
- block_ids: int32 [64, 8, 16], P(None, 'kvh'), may hold values from 0 to 2047, as said below
- block_counts: int32 [2048], P('seq'), may hold values from 64 to 128
- out_weight: bfloat16 [8192, 8192], P('kvh', 'seq'), may hold values from -0.5 to 0.5
Outputs:
- projected: bfloat16 [64, 8192], P('kvh', 'seq')
The draws below stay inside these ranges and needn't reach their ends.
Inputs may be any that keep to these rules, and one draw needn't show every extreme that they name: `block_ids`: for every token and key-value head the 16 ids are different. For every key-value head at most 192 of its 64 x 16 ids lie among the blocks o * 128 to (o + 1) * 128 - 1 of one o, and for some o exactly 192.
All inputs are finite; a program needn't handle non-finite values.
Results may differ from the reference program's by a relative error of at most 0.023.
Values may be sent and summed in bfloat16 or wider, within the bound.
A program may use at most 128 MiB of HBM per device.

```python
import math
import jax
import jax.numpy as jnp
from jax import lax

DM = 8192
H = 64
KVH = 8
HD = 128
BS = 128
R = 4
TOPK = 16
B = 64
BLK_DEV = 128
NB = 2048


def summary_base(key):
    drawn = jax.random.normal(jax.random.fold_in(key, 11), (NB, KVH, R, HD), jnp.float32)
    return jnp.clip(drawn, -6.0, 6.0)


def draw_rep_keys(key, part):
    summary = summary_base(key)
    return summary.astype(jnp.bfloat16)


def draw_queries(key, part):
    query_base = jnp.clip(jax.random.normal(jax.random.fold_in(key, 12), (B, H, HD), jnp.float32), -6.0, 6.0)
    return query_base.astype(jnp.bfloat16)


def draw_block_ids(key, part):
    shards = NB // BLK_DEV
    hot_shard = jax.random.randint(jax.random.fold_in(key, 21), (1, KVH, 1), 0, shards)
    turn_shift = jax.random.randint(jax.random.fold_in(key, 22), (1, KVH, 1), 0, shards - 1)
    token_pos = jnp.arange(B, dtype=jnp.int32).reshape(B, 1, 1)
    slot_pos = jnp.arange(TOPK, dtype=jnp.int32).reshape(1, 1, TOPK)
    spread = (hot_shard + 1 + (token_pos * 13 + slot_pos + turn_shift) % (shards - 1)) % shards
    owners = jnp.where(slot_pos < 3, hot_shard, spread)
    noise = jax.random.randint(jax.random.fold_in(key, 23), (B, KVH, BLK_DEV), 0, 1 << 20)
    ranked = noise * BLK_DEV + jnp.arange(BLK_DEV, dtype=jnp.int32)
    offsets = lax.top_k(ranked, TOPK)[1].astype(jnp.int32)
    picked = owners * BLK_DEV + offsets
    shuffle = jax.random.randint(jax.random.fold_in(key, 24), (B, KVH, TOPK), 0, 1 << 20) * TOPK + jnp.arange(TOPK, dtype=jnp.int32)
    order_ids = lax.top_k(shuffle, TOPK)[1].astype(jnp.int32)
    return jnp.take_along_axis(picked, order_ids, axis=2).astype(jnp.int32)


def plant(values, stream_key, least, high):
    shape = values.shape
    place = [jax.random.randint(jax.random.fold_in(stream_key, axis), (), 0, shape[axis]) for axis in range(len(shape))]
    values = values.at[tuple(place)].set(least)
    longest = shape.index(max(shape))
    place[longest] = (place[longest] + 1) % shape[longest]
    return values.at[tuple(place)].set(high)


def levels(stream_key, extent, pieces, smallest, largest):
    level, own = 1.0, jax.random.fold_in(stream_key, 6)
    for axis_at, blocks in pieces:
        heights = jnp.exp(jax.random.uniform(jax.random.fold_in(own, axis_at), (blocks,), jnp.float32, smallest / len(pieces), largest / len(pieces)))
        level = level * jnp.repeat(heights, extent[axis_at] // blocks).reshape([-1 if axis == axis_at else 1 for axis in range(len(extent))])
    return level


def scatter_about(key, extent, scale, bound, cuts=(), kind=jnp.bfloat16):
    factor_of = levels(key, extent, cuts, -0.22, 0.18) if cuts else 1.0
    array = jax.random.normal(key, extent, jnp.float32) * scale * factor_of
    return jnp.minimum(jnp.maximum(array, -bound), bound).astype(kind)


def setup_inputs(seed: int = 0) -> dict:
    seeds = jax.random.split(jax.random.key(seed), 9)
    queries = draw_queries(jax.random.fold_in(seeds[8], 71), 0)
    keys = scatter_about(seeds[1], (NB, KVH, BS, HD), 1.0, 6.0, ((0, 16), (1, 8)))
    values = scatter_about(seeds[2], (NB, KVH, BS, HD), 1.0, 6.0, ((0, 16), (1, 8)))
    rep_keys = draw_rep_keys(jax.random.fold_in(seeds[8], 71), 0)
    rep_values = scatter_about(seeds[4], (NB, KVH, R, HD), 1.0, 6.0, ((0, 16), (1, 8)))
    block_ids = draw_block_ids(jax.random.fold_in(seeds[8], 71), 0)
    block_counts = plant(jax.random.randint(seeds[6], (NB,), BS // 2, BS + 1), jax.random.fold_in(seeds[6], 1), BS // 2, BS).astype(jnp.int32)
    out_weight = scatter_about(seeds[7], (H * HD, DM), HD ** -0.5, 0.5, ((0, 8), (1, 16)))
    return {"queries": queries, "keys": keys, "values": values, "rep_keys": rep_keys, "rep_values": rep_values, "block_ids": block_ids, "block_counts": block_counts, "out_weight": out_weight}


FLOOR_SCORE = -1e+30

def reference(queries, keys, values, rep_keys, rep_values, block_ids, block_counts, out_weight):
    group_size = H // KVH
    inv_root = 1.0 / math.sqrt(HD)

    def one_head(kv_head):
        query_rows = lax.dynamic_slice_in_dim(queries, kv_head * group_size, group_size, 1).astype(jnp.float32)
        summary_keys = jnp.take(rep_keys, kv_head, axis=1).reshape(NB * R, HD).astype(jnp.float32)
        summary_vals = jnp.take(rep_values, kv_head, axis=1).reshape(NB * R, HD).astype(jnp.float32)
        block_rows = jnp.take(block_ids, kv_head, axis=1)
        tile_keys = keys[block_rows, kv_head].astype(jnp.float32)
        tile_vals = values[block_rows, kv_head].astype(jnp.float32)
        valid_map = jnp.arange(BS, dtype=jnp.int32)[None, None, :] < block_counts[block_rows][:, :, None]
        summary_scores = jnp.einsum('bgd,nd->bgn', query_rows, summary_keys) * inv_root
        chosen_scores = jnp.einsum('bgd,bstd->bgst', query_rows, tile_keys) * inv_root
        chosen_scores = jnp.where(valid_map[:, None], chosen_scores, FLOOR_SCORE)
        highest = jnp.maximum(lax.optimization_barrier(jnp.max(summary_scores, axis=2)), lax.optimization_barrier(jnp.max(chosen_scores, axis=(2, 3))))
        summary_weights = jnp.exp(summary_scores - highest[:, :, None])
        chosen_weights = jnp.where(valid_map[:, None], jnp.exp(chosen_scores - highest[:, :, None, None]), 0.0)
        weight_sum = lax.optimization_barrier(jnp.sum(summary_weights, axis=2)) + lax.optimization_barrier(jnp.sum(chosen_weights, axis=(2, 3)))
        summary_round = lax.optimization_barrier(summary_weights.astype(jnp.bfloat16)).astype(jnp.float32)
        chosen_round = lax.optimization_barrier(chosen_weights.astype(jnp.bfloat16)).astype(jnp.float32)
        weighted = jnp.einsum('bgn,nd->bgd', summary_round, summary_vals)
        weighted = weighted + jnp.einsum('bgst,bstd->bgd', chosen_round, tile_vals)
        return (weighted / weight_sum[:, :, None]).astype(jnp.bfloat16)
    heads_out = lax.map(one_head, jnp.arange(KVH, dtype=jnp.int32))
    attended = jnp.transpose(heads_out, (1, 0, 2, 3)).reshape(B, H * HD)
    return jnp.dot(attended, out_weight, preferred_element_type=jnp.float32).astype(jnp.bfloat16)
```

```python
import functools
import math

import jax
import jax.numpy as jnp
from jax import lax
from jax.experimental import pallas as pl
from jax.experimental.pallas import tpu as pltpu
from jax.sharding import PartitionSpec as P

CAP = 192
UNROLL = 32
FLOOR = -1e30
F32 = jnp.float32
BF16 = jnp.bfloat16
NT = (((1,), (1,)), ((), ()))


def dot(a, b):
    return jnp.dot(a, b, preferred_element_type=F32)


def dot_nt(a, b):
    return lax.dot_general(a, b, NT, preferred_element_type=F32)


def iota(shape, dim):
    return lax.broadcasted_iota(jnp.int32, shape, dim)


def kernel(
    q_hbm, k_hbm, v_hbm, rk_hbm, rv_hbm, ids_hbm, cnt_hbm, w_hbm,
    out_ref,
    q_v, k_v, v_v, rk_v, rv_v, ids_v, w_v, cnt_s, slot_v, slot_s,
    flip, q32, qh_v, score_v, acc_v, summed_v, mg_v, lg_v, seg_v, tmap_v, base_v,
    msum_v, lsum_v, stat_v, send_v, recv_v, piece_v, att_v, psend_v, precv_v,
    in_sem, slot_sem, rs_s, rs_r, ag_s, ag_r, pj_s, pj_r,
):
    seq = lax.axis_index("seq")
    kvh = lax.axis_index("kvh")
    sy, sx = seq // 4, seq % 4
    scale = 1.0 / math.sqrt(128)

    def seq_at(dy, dx):
        return lax.rem(sy + dy + 4, 4) * 4 + lax.rem(sx + dx + 4, 4)

    shifts = [(dy, dx) for dy in range(4) for dx in range(4) if dy or dx]

    barrier = pltpu.get_barrier_semaphore()
    for dy, dx in shifts:
        pl.semaphore_signal(
            barrier, inc=1, device_id={"seq": seq_at(dy, dx)}, device_id_type=pl.DeviceIdType.MESH
        )
    for e in range(1, 8):
        pl.semaphore_signal(
            barrier, inc=1, device_id={"kvh": lax.rem(kvh + e, 8)}, device_id_type=pl.DeviceIdType.MESH
        )

    loads = [
        pltpu.make_async_copy(src, dst, in_sem.at[i])
        for i, (src, dst) in enumerate(
            [
                (ids_hbm, ids_v), (cnt_hbm, cnt_s), (q_hbm, q_v), (rk_hbm, rk_v),
                (rv_hbm, rv_v), (k_hbm, k_v), (v_hbm, v_v), (w_hbm, w_v),
            ]
        )
    ]
    for load in loads:
        load.start()
    l_ids, l_cnt, l_q, l_rk, l_rv, l_k, l_v, l_w = loads

    flip[...] = jnp.zeros_like(flip)
    l_ids.wait()
    flip[0:16, 0:64] = ids_v[...].astype(F32)
    ids = flip[...].T[0:64, :]
    first_id = (seq * 128).astype(F32)
    local = (ids >= first_id) & (ids < first_id + 128.0) & (iota((64, 128), 1) < 16)
    block = ids - first_id
    hit = jnp.where(local, 1.0, 0.0).astype(BF16)
    ones = jnp.ones((128, 128), BF16)
    above = jnp.where(iota((128, 128), 0) < iota((128, 128), 1), 1.0, 0.0).astype(BF16)
    below = jnp.where(iota((64, 64), 1) < iota((64, 64), 0), 1.0, 0.0).astype(BF16)
    base = dot(dot(below, hit).astype(BF16), ones)
    count = dot(hit, ones)
    rank = jnp.where(local, base + dot(hit, above), -1.0)
    slots = iota((64, 256), 1).astype(F32)
    base2 = jnp.concatenate([base, base], axis=1)
    count2 = jnp.concatenate([count, count], axis=1)
    tmap = jnp.where((slots >= base2) & (slots < base2 + count2), 1.0, 0.0)
    first = jnp.where((slots == base2) & (count2 > 0.0), 1.0, 0.0)
    chosen = jnp.zeros((64, 256), F32)
    for s in range(16):
        chosen += jnp.where(rank[:, s : s + 1] == slots, block[:, s : s + 1], 0.0)
    slot_block = jnp.sum(chosen, axis=0, keepdims=True)
    slot_token = jnp.sum(tmap * iota((64, 256), 0).astype(F32), axis=0, keepdims=True)
    slot_live = jnp.sum(tmap, axis=0, keepdims=True)
    seg_v[...] = jnp.broadcast_to(jnp.where(slot_live > 0.0, slot_token, -1.0), (8, 256))
    slot_v[...] = jnp.where(
        iota((8, 256), 0) == 0, slot_token.astype(jnp.int32) & 63, slot_block.astype(jnp.int32) & 127
    )
    tmap_v[0] = tmap.astype(BF16)
    tmap_v[1] = first.astype(BF16)
    base_v[...] = count
    to_smem = pltpu.make_async_copy(slot_v, slot_s, slot_sem)
    to_smem.start()

    l_q.wait()
    q32[0:512, :] = q_v[...].astype(F32).reshape(512, 128)
    for h in range(8):
        qh_v[h * 64 : h * 64 + 64, :] = q32[pl.ds(h, 64, stride=8), :].astype(BF16)
    l_rk.wait()
    l_rv.wait()
    msum_v[...] = jnp.zeros_like(msum_v)
    for c in range(4):
        s = dot_nt(qh_v[c * 128 : c * 128 + 128, :], rk_v[...]) * scale
        m = jnp.max(s, axis=1, keepdims=True).astype(BF16).astype(F32)
        p = jnp.exp(s - m)
        l = jnp.sum(p, axis=1, keepdims=True)
        a = dot(p.astype(BF16), rv_v[...])
        summed_v[c * 128 : c * 128 + 128, :] = a
        for e in range(2):
            h = 2 * c + e
            msum_v[0:64, h : h + 1] = m[e * 64 : e * 64 + 64]
            lsum_v[:, h : h + 1] = l[e * 64 : e * 64 + 64]

    lane = iota((8, 128), 1)
    l_cnt.wait()
    to_smem.wait()
    l_k.wait()

    def score(g, carry):
        for half in range(UNROLL // 16):
            top = jnp.zeros((8, 128), F32)
            for u in range(16):
                j = g * UNROLL + half * 16 + u
                blk = slot_s[1, j]
                s = dot_nt(q_v[slot_s[0, j]], k_v[blk]) * scale
                s = jnp.where(lane < cnt_s[blk], s, FLOOR)
                score_v[j] = s
                top = jnp.where(lane == u, jnp.max(s, axis=1, keepdims=True), top)
            mg_v[g * (UNROLL // 16) + half] = top
        return carry

    lax.fori_loop(0, CAP // UNROLL, score, 0)

    def gathered(ref):
        sides = []
        for side in range(2):
            found = jnp.zeros((8, 128), F32)
            for i in range(8):
                g = side * 8 + i
                if g < CAP // 16:
                    part = ref[g] if i == 0 else pltpu.roll(ref[g], i * 16, 1)
                    found = jnp.where((lane >= i * 16) & (lane < i * 16 + 16), part, found)
            sides.append(found)
        return jnp.concatenate(sides, axis=1)

    top = gathered(mg_v).astype(BF16).astype(F32)
    token = seg_v[...]
    for back in (False, True):
        for k in (1, 2, 4, 8):
            by = 256 - k if back else k
            same = pltpu.roll(token, by, 1) == token
            top = jnp.maximum(top, jnp.where(same, pltpu.roll(top, by, 1), FLOOR))
    tmap_b, first_b = tmap_v[0], tmap_v[1]
    msum = msum_v[...]
    sum_top = dot(msum.T[0:8, 0:64].astype(BF16), tmap_b)
    top = jnp.maximum(top, sum_top)
    for g in range(CAP // 16):
        part = top[:, (g // 8) * 128 : (g // 8) * 128 + 128]
        mg_v[g] = part if g % 8 == 0 else pltpu.roll(part, 128 - (g % 8) * 16, 1)

    l_v.wait()

    def weigh(g, carry):
        for half in range(UNROLL // 16):
            i = g * (UNROLL // 16) + half
            tops = mg_v[i]
            total = jnp.zeros((8, 128), F32)
            for u in range(16):
                j = g * UNROLL + half * 16 + u
                p = jnp.exp(score_v[j] - tops[:, u : u + 1])
                total = jnp.where(lane == u, jnp.sum(p, axis=1, keepdims=True), total)
                acc_v[pl.ds(j, 8, stride=CAP), :] = dot(p.astype(BF16), v_v[slot_s[1, j]])
            lg_v[i] = total
        return carry

    lax.fori_loop(0, CAP // UNROLL, weigh, 0)

    total = gathered(lg_v)
    total_hi = total.astype(BF16)
    total_lo = (total - total_hi.astype(F32)).astype(BF16)
    sums = dot_nt(tmap_b, total_hi) + dot_nt(tmap_b, total_lo)
    sum_m = msum[0:64, 0:8]
    high = jnp.where(base_v[:, 0:8] > 0.0, dot_nt(first_b, top.astype(BF16)), sum_m)
    factor = jnp.exp(sum_m - high)
    sums = sums + lsum_v[:, 0:8] * factor
    sums_hi = sums.astype(BF16).astype(F32)
    stat_v[...] = jnp.zeros_like(stat_v)
    stat_v[:, 0:8] = high
    stat_v[:, 8:16] = sums_hi
    stat_v[:, 16:24] = sums - sums_hi
    stat = stat_v[...].astype(BF16)
    for o in range(16):
        t = o % 4
        send_v[o, 2] = stat[t * 16 : t * 16 + 16]
    tmap_c = tmap_b[:, 0:CAP]
    for h in range(8):
        a = dot(tmap_c, acc_v[h * CAP : h * CAP + CAP, :].astype(BF16))
        a = a + summed_v[h * 64 : h * 64 + 64, :] * factor[:, h : h + 1]
        a = a.astype(BF16)
        for t in range(4):
            send_v[(h // 2) * 4 + t, h % 2] = a[t * 16 : t * 16 + 16]

    pl.semaphore_wait(barrier, 22)

    def remote(src, dst, send_sem, recv_sem, where):
        return pltpu.make_async_remote_copy(
            src_ref=src, dst_ref=dst, send_sem=send_sem, recv_sem=recv_sem,
            device_id=where, device_id_type=pl.DeviceIdType.MESH,
        )

    order = sorted(shifts, key=lambda d: -(min(d[0], 4 - d[0]) + min(d[1], 4 - d[1])))
    pushes = []
    for dy, dx in order:
        d = dy * 4 + dx
        peer = seq_at(dy, dx)
        pushes.append(
            remote(send_v.at[peer], recv_v.at[d], rs_s.at[d], rs_r.at[d], {"seq": peer})
        )
        pushes[-1].start()
    recv_v[0] = send_v[seq]
    for push in pushes:
        push.wait_recv()
    stats = [recv_v[d, 2].astype(F32) for d in range(16)]
    high = functools.reduce(jnp.maximum, stats)
    factors = [jnp.exp(x - high) for x in stats]
    whole = sum(
        f * (pltpu.roll(x, 120, 1) + pltpu.roll(x, 112, 1)) for f, x in zip(factors, stats)
    )
    mine = 2 * (seq // 4)
    column = iota((16, 128), 1)
    heads = [jnp.zeros((16, 128), F32) for _ in range(2)]
    for d in range(16):
        share = factors[d] / whole
        for e in range(2):
            g = jnp.sum(jnp.where(column == mine + e, share, 0.0), axis=1, keepdims=True)
            heads[e] = heads[e] + recv_v[d, e].astype(F32) * g
    for e in range(2):
        piece_v[e] = heads[e].astype(BF16)

    def place(o):
        return att_v.at[pl.ds(2 * (o // 4), 2), pl.ds(pl.multiple_of(16 * (o % 4), 16), 16), :]

    spreads = []
    for dy, dx in order:
        d = dy * 4 + dx
        peer = seq_at(dy, dx)
        spread = remote(piece_v, place(seq), ag_s.at[d], ag_r.at[d], {"seq": peer})
        spread.start()
        spreads.append((dy, dx, spread))
    place(seq)[...] = piece_v[...]
    for push in pushes:
        push.wait_send()
    l_w.wait()
    for dy, dx, spread in spreads:
        d = dy * 4 + dx
        source = seq_at(-dy, -dx)
        remote(piece_v, place(source), ag_s.at[d], ag_r.at[d], {"seq": source}).wait_recv()

    terms = dot(att_v[0], w_v[0:128, :])
    for h in range(1, 8):
        terms += dot(att_v[h], w_v[h * 128 : h * 128 + 128, :])
    for e in range(8):
        psend_v[e] = terms[e * 8 : e * 8 + 8, :].astype(BF16)
    hands = []
    for e in (4, 5, 3, 6, 2, 7, 1):
        peer = lax.rem(kvh + e, 8)
        hand = remote(psend_v.at[peer], precv_v.at[e], pj_s.at[e], pj_r.at[e], {"kvh": peer})
        hand.start()
        hands.append(hand)
    for _, _, spread in spreads:
        spread.wait_send()
    result = psend_v[kvh].astype(F32)
    for hand in hands:
        hand.wait_recv()
    for e in range(1, 8):
        result = result + precv_v[e].astype(F32)
    out_ref[...] = result.astype(BF16)
    for hand in hands:
        hand.wait_send()


def on_device(queries, keys, values, rep_keys, rep_values, block_ids, block_counts, out_weight):
    vmem, smem, dma = pltpu.VMEM, pltpu.SMEM, pltpu.SemaphoreType.DMA
    any_spec = pl.BlockSpec(memory_space=pl.ANY)
    return pl.pallas_call(
        kernel,
        out_shape=jax.ShapeDtypeStruct((8, 512), BF16),
        in_specs=[any_spec] * 8,
        out_specs=pl.BlockSpec(memory_space=pltpu.VMEM),
        scratch_shapes=[
            vmem((64, 8, 128), BF16), vmem((128, 128, 128), BF16), vmem((128, 128, 128), BF16),
            vmem((512, 128), BF16), vmem((512, 128), BF16), vmem((16, 64), jnp.int32),
            vmem((1024, 512), BF16), smem((128,), jnp.int32), vmem((8, 256), jnp.int32),
            smem((8, 256), jnp.int32),
            vmem((128, 128), F32), vmem((520, 128), F32), vmem((512, 128), BF16),
            vmem((CAP, 8, 128), F32), vmem((9 * CAP, 128), F32), vmem((512, 128), F32),
            vmem((CAP // 16, 8, 128), F32), vmem((CAP // 16, 8, 128), F32), vmem((8, 256), F32),
            vmem((2, 64, 256), BF16), vmem((64, 128), F32),
            vmem((128, 128), F32), vmem((64, 128), F32), vmem((64, 128), F32),
            vmem((16, 3, 16, 128), BF16), vmem((16, 3, 16, 128), BF16), vmem((2, 16, 128), BF16),
            vmem((8, 64, 128), BF16), vmem((8, 8, 512), BF16), vmem((8, 8, 512), BF16),
            dma((8,)), dma, dma((16,)), dma((16,)), dma((16,)), dma((16,)), dma((8,)), dma((8,)),
        ],
        compiler_params=pltpu.CompilerParams(collective_id=0, has_side_effects=True),
        name="decode",
    )(
        queries,
        keys.reshape(keys.shape[0], keys.shape[2], keys.shape[3]),
        values.reshape(values.shape[0], values.shape[2], values.shape[3]),
        rep_keys.reshape(-1, rep_keys.shape[3]),
        rep_values.reshape(-1, rep_values.shape[3]),
        jnp.transpose(block_ids, (1, 2, 0)).reshape(block_ids.shape[2], block_ids.shape[0]),
        block_counts,
        out_weight,
    )


def solution(mesh):
    in_specs = (
        P(None, "kvh", None),
        P("seq", "kvh", None, None),
        P("seq", "kvh", None, None),
        P("seq", "kvh", None, None),
        P("seq", "kvh", None, None),
        P(None, "kvh", None),
        P("seq"),
        P("kvh", "seq"),
    )
    return jax.shard_map(
        on_device, mesh=mesh, in_specs=in_specs, out_specs=P("kvh", "seq"), check_vma=False
    )
```

```python
import functools
import math

import jax
import jax.numpy as jnp
from jax import lax
from jax.experimental import pallas as pl
from jax.experimental.pallas import tpu as pltpu
from jax.sharding import PartitionSpec as P

CAP = 192
UNROLL = 192
STRIDE = 196
FLOOR = -1e30
F32 = jnp.float32
BF16 = jnp.bfloat16
NT = (((1,), (1,)), ((), ()))


def dot(a, b):
    return jnp.dot(a, b, preferred_element_type=F32)


def dot_nt(a, b):
    return lax.dot_general(a, b, NT, preferred_element_type=F32)


def iota(shape, dim):
    return lax.broadcasted_iota(jnp.int32, shape, dim)


def kernel(
    q_hbm, k_hbm, v_hbm, rk_hbm, rv_hbm, ids_hbm, cnt_hbm, w_hbm,
    out_ref,
    q_v, k_v, v_v, rk_v, rv_v, ids_v, w_v, cnt_s, slot_v, slot_s,
    flip, q3, q32, qh_v, score_v, acc_v, summed_v, mg_v, lg_v, seg_v, tmap_v, base_v,
    msum_v, lsum_v, stat_v, send_v, recv_v, piece_v, att_v, psend_v, precv_v,
    in_sem, slot_sem, rs_s, rs_r, ag_s, ag_r, pj_s, pj_r,
):
    seq = lax.axis_index("seq")
    kvh = lax.axis_index("kvh")
    sy, sx = seq // 4, seq % 4
    scale = 1.0 / math.sqrt(128)

    def seq_at(dy, dx):
        return lax.rem(sy + dy + 4, 4) * 4 + lax.rem(sx + dx + 4, 4)

    shifts = [(dy, dx) for dy in range(4) for dx in range(4) if dy or dx]

    barrier = pltpu.get_barrier_semaphore()
    for dy, dx in shifts:
        pl.semaphore_signal(
            barrier, inc=1, device_id={"seq": seq_at(dy, dx)}, device_id_type=pl.DeviceIdType.MESH
        )
    for e in range(1, 8):
        pl.semaphore_signal(
            barrier, inc=1, device_id={"kvh": lax.rem(kvh + e, 8)}, device_id_type=pl.DeviceIdType.MESH
        )

    loads = [
        pltpu.make_async_copy(src, dst, in_sem.at[i])
        for i, (src, dst) in enumerate(
            [
                (ids_hbm, ids_v), (cnt_hbm, cnt_s), (q_hbm, q_v), (rk_hbm, rk_v),
                (rv_hbm, rv_v), (k_hbm, k_v), (v_hbm, v_v), (w_hbm, w_v),
            ]
        )
    ]
    for load in loads:
        load.start()
    l_ids, l_cnt, l_q, l_rk, l_rv, l_k, l_v, l_w = loads

    flip[...] = jnp.zeros_like(flip)
    with jax.named_scope("wait_ids"):
        l_ids.wait()
    flip[0:16, 0:64] = ids_v[...].astype(F32)
    ids = flip[...].T[0:64, :]
    first_id = (seq * 128).astype(F32)
    local = (ids >= first_id) & (ids < first_id + 128.0) & (iota((64, 128), 1) < 16)
    block = ids - first_id
    hit = jnp.where(local, 1.0, 0.0).astype(BF16)
    ones = jnp.ones((128, 128), BF16)
    above = jnp.where(iota((128, 128), 0) < iota((128, 128), 1), 1.0, 0.0).astype(BF16)
    below = jnp.where(iota((64, 64), 1) < iota((64, 64), 0), 1.0, 0.0).astype(BF16)
    base = dot(dot(below, hit).astype(BF16), ones)
    count = dot(hit, ones)
    rank = jnp.where(local, base + dot(hit, above), -1.0)
    slots = iota((64, 256), 1).astype(F32)
    base2 = jnp.concatenate([base, base], axis=1)
    count2 = jnp.concatenate([count, count], axis=1)
    tmap = jnp.where((slots >= base2) & (slots < base2 + count2), 1.0, 0.0)
    first = jnp.where((slots == base2) & (count2 > 0.0), 1.0, 0.0)
    chosen = jnp.zeros((64, 256), F32)
    for s in range(16):
        chosen += jnp.where(rank[:, s : s + 1] == slots, block[:, s : s + 1], 0.0)
    slot_block = jnp.sum(chosen, axis=0, keepdims=True)
    slot_token = jnp.sum(tmap * iota((64, 256), 0).astype(F32), axis=0, keepdims=True)
    slot_live = jnp.sum(tmap, axis=0, keepdims=True)
    seg_v[...] = jnp.broadcast_to(jnp.where(slot_live > 0.0, slot_token, -1.0), (8, 256))
    slot_v[...] = jnp.where(
        iota((8, 256), 0) == 0, slot_token.astype(jnp.int32) & 63, slot_block.astype(jnp.int32) & 127
    )
    tmap_v[0] = tmap.astype(BF16)
    tmap_v[1] = first.astype(BF16)
    base_v[...] = count
    to_smem = pltpu.make_async_copy(slot_v, slot_s, slot_sem)
    to_smem.start()

    with jax.named_scope("wait_q"):
        l_q.wait()
    wide = q_v[...].astype(F32)
    q3[...] = wide
    q32[0:512, :] = wide.reshape(512, 128)
    for h in range(8):
        qh_v[h * 64 : h * 64 + 64, :] = q32[pl.ds(h, 64, stride=8), :].astype(BF16)
    with jax.named_scope("wait_rep"):
        l_rk.wait()
        l_rv.wait()
    msum_v[...] = jnp.zeros_like(msum_v)
    for c in range(4):
        s = dot_nt(qh_v[c * 128 : c * 128 + 128, :], rk_v[...]) * scale
        m = jnp.max(s, axis=1, keepdims=True).astype(BF16).astype(F32)
        p = jnp.exp(s - m)
        l = jnp.sum(p, axis=1, keepdims=True)
        a = dot(p.astype(BF16), rv_v[...])
        summed_v[c * 128 : c * 128 + 128, :] = a
        for e in range(2):
            h = 2 * c + e
            msum_v[0:64, h : h + 1] = m[e * 64 : e * 64 + 64]
            lsum_v[:, h : h + 1] = l[e * 64 : e * 64 + 64]

    lane = iota((8, 128), 1)
    with jax.named_scope("wait_k"):
        l_cnt.wait()
        to_smem.wait()
        l_k.wait()

    empty = jnp.zeros((8, 128), F32)

    def beside(a, b):
        return jnp.concatenate([a, b], axis=1)

    def four(a, b, c, d):
        rows = [beside(a, empty), beside(empty, b), beside(c, empty), beside(empty, d)]
        return jnp.concatenate(rows, axis=0).astype(BF16)

    def apart(r):
        return r[0:8, 0:128], r[8:16, 0:128], r[16:24, 128:256], r[24:32, 128:256]

    def query(j):
        return q3[slot_s[0, j]]

    def score(g, carry):
        for half in range(UNROLL // 16):
            top = jnp.zeros((8, 128), F32)
            for u in range(0, 16, 4):
                j = g * UNROLL + half * 16 + u
                blk = [slot_s[1, j + i] for i in range(4)]
                tile = [k_v[blk[i]] for i in range(4)]
                tile = jnp.concatenate([beside(tile[0], tile[1]), beside(tile[2], tile[3])], axis=0)
                found = apart(dot_nt(four(*[query(j + i) for i in range(4)]), tile))
                for i in range(4):
                    s = jnp.where(lane < cnt_s[blk[i]], found[i] * scale, FLOOR)
                    score_v[j + i] = s
                    top = jnp.where(lane == u + i, jnp.max(s, axis=1, keepdims=True), top)
            mg_v[g * (UNROLL // 16) + half] = top
        return carry

    with jax.named_scope("score"):
        lax.fori_loop(0, CAP // UNROLL, score, 0)

    def gathered(ref):
        sides = []
        for side in range(2):
            found = jnp.zeros((8, 128), F32)
            for i in range(8):
                g = side * 8 + i
                if g < CAP // 16:
                    part = ref[g] if i == 0 else pltpu.roll(ref[g], i * 16, 1)
                    found = jnp.where((lane >= i * 16) & (lane < i * 16 + 16), part, found)
            sides.append(found)
        return jnp.concatenate(sides, axis=1)

    top = gathered(mg_v).astype(BF16).astype(F32)
    token = seg_v[...]
    for back in (False, True):
        for k in (1, 2, 4, 8):
            by = 256 - k if back else k
            same = pltpu.roll(token, by, 1) == token
            top = jnp.maximum(top, jnp.where(same, pltpu.roll(top, by, 1), FLOOR))
    tmap_b, first_b = tmap_v[0], tmap_v[1]
    msum = msum_v[...]
    sum_top = dot(msum.T[0:8, 0:64].astype(BF16), tmap_b)
    top = jnp.maximum(top, sum_top)
    for g in range(CAP // 16):
        part = top[:, (g // 8) * 128 : (g // 8) * 128 + 128]
        mg_v[g] = part if g % 8 == 0 else pltpu.roll(part, 128 - (g % 8) * 16, 1)

    with jax.named_scope("wait_v"):
        l_v.wait()

    def weigh(g, carry):
        for half in range(UNROLL // 16):
            at = g * (UNROLL // 16) + half
            tops = mg_v[at]
            total = jnp.zeros((8, 128), F32)
            for u in range(0, 16, 4):
                j = g * UNROLL + half * 16 + u
                ps = []
                for i in range(4):
                    p = jnp.exp(score_v[j + i] - tops[:, u + i : u + i + 1])
                    total = jnp.where(lane == u + i, jnp.sum(p, axis=1, keepdims=True), total)
                    ps.append(p)
                tile = [v_v[slot_s[1, j + i]] for i in range(4)]
                tile = jnp.concatenate([beside(tile[0], tile[2]), beside(tile[1], tile[3])], axis=0)
                found = apart(dot(four(*ps), tile))
                for i in range(4):
                    acc_v[pl.ds(j + i, 8, stride=STRIDE), :] = found[i]
            lg_v[at] = total
        return carry

    with jax.named_scope("weigh"):
        lax.fori_loop(0, CAP // UNROLL, weigh, 0)

    total = gathered(lg_v)
    total_hi = total.astype(BF16)
    total_lo = (total - total_hi.astype(F32)).astype(BF16)
    sums = dot_nt(tmap_b, total_hi) + dot_nt(tmap_b, total_lo)
    sum_m = msum[0:64, 0:8]
    high = jnp.where(base_v[:, 0:8] > 0.0, dot_nt(first_b, top.astype(BF16)), sum_m)
    factor = jnp.exp(sum_m - high)
    sums = sums + lsum_v[:, 0:8] * factor
    sums_hi = sums.astype(BF16).astype(F32)
    stat_v[...] = jnp.zeros_like(stat_v)
    stat_v[:, 0:8] = high
    stat_v[:, 8:16] = sums_hi
    stat_v[:, 16:24] = sums - sums_hi
    stat = stat_v[...].astype(BF16)
    for o in range(16):
        t = o % 4
        send_v[o, 2] = stat[t * 16 : t * 16 + 16]
    tmap_c = tmap_b[:, 0:CAP]
    for h in range(8):
        a = dot(tmap_c, acc_v[h * STRIDE : h * STRIDE + CAP, :].astype(BF16))
        a = a + summed_v[h * 64 : h * 64 + 64, :] * factor[:, h : h + 1]
        a = a.astype(BF16)
        for t in range(4):
            send_v[(h // 2) * 4 + t, h % 2] = a[t * 16 : t * 16 + 16]

    with jax.named_scope("barrier"):
        pl.semaphore_wait(barrier, 22)

    def remote(src, dst, send_sem, recv_sem, where):
        return pltpu.make_async_remote_copy(
            src_ref=src, dst_ref=dst, send_sem=send_sem, recv_sem=recv_sem,
            device_id=where, device_id_type=pl.DeviceIdType.MESH,
        )

    order = sorted(shifts, key=lambda d: -(min(d[0], 4 - d[0]) + min(d[1], 4 - d[1])))
    pushes = []
    for dy, dx in order:
        d = dy * 4 + dx
        peer = seq_at(dy, dx)
        pushes.append(
            remote(send_v.at[peer], recv_v.at[d], rs_s.at[d], rs_r.at[d], {"seq": peer})
        )
        pushes[-1].start()
    recv_v[0] = send_v[seq]
    with jax.named_scope("rs_recv"):
        for push in pushes:
            push.wait_recv()
    stats = [recv_v[d, 2].astype(F32) for d in range(16)]
    high = functools.reduce(jnp.maximum, stats)
    factors = [jnp.exp(x - high) for x in stats]
    whole = sum(
        f * (pltpu.roll(x, 120, 1) + pltpu.roll(x, 112, 1)) for f, x in zip(factors, stats)
    )
    mine = 2 * (seq // 4)
    column = iota((16, 128), 1)
    heads = [jnp.zeros((16, 128), F32) for _ in range(2)]
    for d in range(16):
        share = factors[d] / whole
        for e in range(2):
            g = jnp.sum(jnp.where(column == mine + e, share, 0.0), axis=1, keepdims=True)
            heads[e] = heads[e] + recv_v[d, e].astype(F32) * g
    for e in range(2):
        piece_v[e] = heads[e].astype(BF16)

    def place(o):
        return att_v.at[pl.ds(2 * (o // 4), 2), pl.ds(pl.multiple_of(16 * (o % 4), 16), 16), :]

    spreads = []
    for dy, dx in order:
        d = dy * 4 + dx
        peer = seq_at(dy, dx)
        spread = remote(piece_v, place(seq), ag_s.at[d], ag_r.at[d], {"seq": peer})
        spread.start()
        spreads.append((dy, dx, spread))
    place(seq)[...] = piece_v[...]
    with jax.named_scope("ag_wait_send"):
        for push in pushes:
            push.wait_send()
        l_w.wait()
    with jax.named_scope("ag_recv"):
        for dy, dx, spread in spreads:
            d = dy * 4 + dx
            source = seq_at(-dy, -dx)
            remote(piece_v, place(source), ag_s.at[d], ag_r.at[d], {"seq": source}).wait_recv()

    terms = dot(att_v[0], w_v[0:128, :])
    for h in range(1, 8):
        terms += dot(att_v[h], w_v[h * 128 : h * 128 + 128, :])
    for e in range(8):
        psend_v[e] = terms[e * 8 : e * 8 + 8, :].astype(BF16)
    hands = []
    for e in (4, 5, 3, 6, 2, 7, 1):
        peer = lax.rem(kvh + e, 8)
        hand = remote(psend_v.at[peer], precv_v.at[e], pj_s.at[e], pj_r.at[e], {"kvh": peer})
        hand.start()
        hands.append(hand)
    for _, _, spread in spreads:
        spread.wait_send()
    result = psend_v[kvh].astype(F32)
    with jax.named_scope("pj_recv"):
        for hand in hands:
            hand.wait_recv()
    for e in range(1, 8):
        result = result + precv_v[e].astype(F32)
    out_ref[...] = result.astype(BF16)
    with jax.named_scope("pj_send"):
        for hand in hands:
            hand.wait_send()


def on_device(queries, keys, values, rep_keys, rep_values, block_ids, block_counts, out_weight):
    vmem, smem, dma = pltpu.VMEM, pltpu.SMEM, pltpu.SemaphoreType.DMA
    any_spec = pl.BlockSpec(memory_space=pl.ANY)
    return pl.pallas_call(
        kernel,
        out_shape=jax.ShapeDtypeStruct((8, 512), BF16),
        in_specs=[any_spec] * 8,
        out_specs=pl.BlockSpec(memory_space=pltpu.VMEM),
        scratch_shapes=[
            vmem((64, 8, 128), BF16), vmem((128, 128, 128), BF16), vmem((128, 128, 128), BF16),
            vmem((512, 128), BF16), vmem((512, 128), BF16), vmem((16, 64), jnp.int32),
            vmem((1024, 512), BF16), smem((128,), jnp.int32), vmem((8, 256), jnp.int32),
            smem((8, 256), jnp.int32),
            vmem((128, 128), F32), vmem((64, 8, 128), F32), vmem((520, 128), F32), vmem((512, 128), BF16),
            vmem((CAP, 8, 128), F32), vmem((9 * STRIDE, 128), F32), vmem((512, 128), F32),
            vmem((CAP // 16, 8, 128), F32), vmem((CAP // 16, 8, 128), F32), vmem((8, 256), F32),
            vmem((2, 64, 256), BF16), vmem((64, 128), F32),
            vmem((128, 128), F32), vmem((64, 128), F32), vmem((64, 128), F32),
            vmem((16, 3, 16, 128), BF16), vmem((16, 3, 16, 128), BF16), vmem((2, 16, 128), BF16),
            vmem((8, 64, 128), BF16), vmem((8, 8, 512), BF16), vmem((8, 8, 512), BF16),
            dma((8,)), dma, dma((16,)), dma((16,)), dma((16,)), dma((16,)), dma((8,)), dma((8,)),
        ],
        compiler_params=pltpu.CompilerParams(collective_id=0, has_side_effects=True),
        name="decode",
    )(
        queries,
        keys.reshape(keys.shape[0], keys.shape[2], keys.shape[3]),
        values.reshape(values.shape[0], values.shape[2], values.shape[3]),
        rep_keys.reshape(-1, rep_keys.shape[3]),
        rep_values.reshape(-1, rep_values.shape[3]),
        jnp.transpose(block_ids, (1, 2, 0)).reshape(block_ids.shape[2], block_ids.shape[0]),
        block_counts,
        out_weight,
    )


def solution(mesh):
    in_specs = (
        P(None, "kvh", None),
        P("seq", "kvh", None, None),
        P("seq", "kvh", None, None),
        P("seq", "kvh", None, None),
        P("seq", "kvh", None, None),
        P(None, "kvh", None),
        P("seq"),
        P("kvh", "seq"),
    )
    return jax.shard_map(
        on_device, mesh=mesh, in_specs=in_specs, out_specs=P("kvh", "seq"), check_vma=False
    )
```

```python
import functools
import math

import jax
import jax.numpy as jnp
from jax import lax
from jax.experimental import pallas as pl
from jax.experimental.pallas import tpu as pltpu
from jax.sharding import PartitionSpec as P

CAP = 192
STRIDE = 196
FLOOR = -1e30
F32 = jnp.float32
BF16 = jnp.bfloat16
NT = (((1,), (1,)), ((), ()))


def dot(a, b):
    return jnp.dot(a, b, preferred_element_type=F32)


def dot_nt(a, b):
    return lax.dot_general(a, b, NT, preferred_element_type=F32)


def iota(shape, dim):
    return lax.broadcasted_iota(jnp.int32, shape, dim)


def kernel(
    q_hbm, k_hbm, v_hbm, rk_hbm, rv_hbm, ids_hbm, cnt_hbm, w_hbm,
    out_ref,
    q_v, k_v, v_v, rk_v, rv_v, ids_v, w_v, cnt_s, slot_v, slot_s,
    wide_v, q3, q32, qh_v, rs_v, rp_v, weight_v, acc_v, summed_v, seg_v,
    tmap_v, col_v, row_v, cnt_v, send_v, recv_v, zsend_v, zrecv_v, piece_v, att_v, psend_v, precv_v,
    in_sem, slot_sem, rs_s, rs_r, rz_s, rz_r, ag_s, ag_r, pj_s, pj_r,
):
    seq = lax.axis_index("seq")
    kvh = lax.axis_index("kvh")
    sy, sx = seq // 4, seq % 4
    scale = 1.0 / math.sqrt(128)

    def seq_at(dy, dx):
        return lax.rem(sy + dy + 4, 4) * 4 + lax.rem(sx + dx + 4, 4)

    shifts = [(dy, dx) for dy in range(4) for dx in range(4) if dy or dx]

    barrier = pltpu.get_barrier_semaphore()
    loads = [
        pltpu.make_async_copy(src, dst, in_sem.at[i])
        for i, (src, dst) in enumerate(
            [
                (ids_hbm, ids_v), (cnt_hbm, cnt_s), (q_hbm, q_v), (rk_hbm, rk_v),
                (rv_hbm, rv_v), (k_hbm, k_v), (v_hbm, v_v), (w_hbm, w_v),
            ]
        )
    ]
    for load in loads:
        load.start()
    l_ids, l_cnt, l_q, l_rk, l_rv, l_k, l_v, l_w = loads
    for dy, dx in shifts:
        pl.semaphore_signal(
            barrier, inc=1, device_id={"seq": seq_at(dy, dx)}, device_id_type=pl.DeviceIdType.MESH
        )
    for e in range(1, 8):
        pl.semaphore_signal(
            barrier, inc=1, device_id={"kvh": lax.rem(kvh + e, 8)}, device_id_type=pl.DeviceIdType.MESH
        )

    def where_true(cond):
        return jnp.where(cond, 1.0, 0.0).astype(BF16)

    wide_v[...] = jnp.full_like(wide_v, -1.0)
    col_v[...] = jnp.zeros_like(col_v)
    slot_v[...] = jnp.zeros_like(slot_v)
    with jax.named_scope("wait_ids"):
        l_ids.wait()
    wide_v[:, 0:64] = ids_v[...].astype(F32)
    ids = wide_v[...]
    first_id = (seq * 128).astype(F32)
    local = (ids >= first_id) & (ids < first_id + 128.0)
    block = ids - first_id
    hit = where_true(local)
    before = where_true(iota((16, 16), 1) < iota((16, 16), 0))
    counts = dot(jnp.ones((256, 16), BF16), hit)
    earlier = where_true(iota((128, 128), 0) < iota((128, 128), 1))
    rank = dot(counts[0:16].astype(BF16), earlier) + dot(before, hit)
    rank = jnp.where(local, rank, -1.0).astype(jnp.int32)
    high, low = rank >> 4, rank & 15
    digit = iota((16, 128), 0)
    token_at = iota((16, 128), 1).astype(F32)
    blocks, tokens, lows = [], [], []
    for s in range(16):
        same = high[s : s + 1, :] == digit
        blocks.append(jnp.where(same, block[s : s + 1, :], 0.0))
        tokens.append(jnp.where(same, token_at, 0.0))
        lows.append(jnp.where(low[s : s + 1, :] == digit, 1.0, 0.0))
    chosen = [jnp.concatenate(x, axis=1).astype(BF16) for x in (blocks, tokens, lows)]
    slots = dot_nt(chosen[2], jnp.concatenate(chosen[0:2], axis=0)).astype(jnp.int32)
    slot_v[:, 0:32] = slots & jnp.where(iota((16, 32), 1) < 16, 127, 63)
    to_smem = pltpu.make_async_copy(slot_v, slot_s, slot_sem)
    to_smem.start()
    cnt_v[...] = counts[0:8]
    counts = counts.astype(BF16)
    base = dot_nt(where_true(iota((64, 128), 1) < iota((64, 128), 0)), counts)
    count = dot_nt(where_true(iota((64, 128), 1) == iota((64, 128), 0)), counts)
    at = iota((64, 256), 1).astype(F32)
    tmap = jnp.where((at >= base) & (at < base + count), 1.0, 0.0)
    slot_token = jnp.sum(tmap * (iota((64, 256), 0) + 1).astype(F32), axis=0, keepdims=True)
    seg_v[...] = jnp.broadcast_to(slot_token, (8, 256))
    tmap_v[0] = tmap.astype(BF16)
    tmap_v[1] = where_true((at == base) & (count > 0.0))
    tmap_v[2] = where_true(count > 0.0)

    with jax.named_scope("wait_q"):
        l_q.wait()
        l_rk.wait()
        l_rv.wait()
    wide = q_v[...].astype(F32)
    q3[...] = wide
    q32[0:512, :] = wide.reshape(512, 128)
    for h in range(8):
        qh_v[h * 64 : h * 64 + 64, :] = q32[pl.ds(h, 64, stride=8), :].astype(BF16)
    rs_v[...] = dot_nt(qh_v[...], rk_v[...])
    for h in range(8):
        s = rs_v[h * 64 : h * 64 + 64, :] * scale
        m = jnp.max(s, axis=1, keepdims=True)
        p = jnp.exp(s - m)
        rp_v[h * 64 : h * 64 + 64, :] = p.astype(BF16)
        col_v[0:64, h : h + 1] = m
        col_v[0:64, 8 + h : 9 + h] = jnp.sum(p, axis=1, keepdims=True)
    summed_v[...] = dot(rp_v[...], rv_v[...])
    row_v[...] = col_v[...].T[0:16, :]

    lane = iota((8, 128), 1)
    empty = jnp.zeros((8, 128), F32)

    def beside(a, b):
        return jnp.concatenate([a, b], axis=1)

    def four(a, b, c, d):
        rows = [beside(a, empty), beside(empty, b), beside(c, empty), beside(empty, d)]
        return jnp.concatenate(rows, axis=0).astype(BF16)

    def apart(r):
        return r[0:8, 0:128], r[8:16, 0:128], r[16:24, 128:256], r[24:32, 128:256]

    with jax.named_scope("wait_smem"):
        l_cnt.wait()
        to_smem.wait()
    with jax.named_scope("wait_k"):
        l_k.wait()
    tops, totals = [empty, empty], [empty, empty]
    for j in range(0, CAP, 4):
        own = range(4)
        half = j // 128
        blk = [slot_s[j % 16 + i, j // 16] for i in own]
        query = [q3[slot_s[j % 16 + i, 16 + j // 16]] for i in own]
        tile = [k_v[blk[i]] for i in own]
        tile = jnp.concatenate([beside(tile[0], tile[1]), beside(tile[2], tile[3])], axis=0)
        found = apart(dot_nt(four(*query), tile))
        ps = []
        for i in own:
            here = lane == (j + i) % 128
            s = jnp.where(lane < cnt_s[blk[i]], found[i] * scale, FLOOR)
            m = jnp.max(s, axis=1, keepdims=True)
            p = jnp.exp(s - m)
            tops[half] = jnp.where(here, m, tops[half])
            totals[half] = jnp.where(here, jnp.sum(p, axis=1, keepdims=True), totals[half])
            ps.append(p)
        weight_v[j // 4] = four(*ps)
    with jax.named_scope("wait_v"):
        l_v.wait()
    for j in range(0, CAP, 4):
        tile = [v_v[slot_s[j % 16 + i, j // 16]] for i in own]
        tile = jnp.concatenate([beside(tile[0], tile[2]), beside(tile[1], tile[3])], axis=0)
        found = apart(dot(weight_v[j // 4], tile))
        for i in own:
            acc_v[pl.ds(j + i, 8, stride=STRIDE), :] = found[i]

    top, total = beside(*tops), beside(*totals)
    token = seg_v[...]
    most = top
    for back in (False, True):
        for k in (1, 2, 4, 8):
            by = 256 - k if back else k
            same = pltpu.roll(token, by, 1) == token
            most = jnp.maximum(most, jnp.where(same, pltpu.roll(most, by, 1), FLOOR))
    tmap_b, first_b = tmap_v[0], tmap_v[1]
    sum_m, sum_l = row_v[0:8, 0:64], row_v[8:16, 0:64]
    most = jnp.maximum(most, dot(sum_m.astype(BF16), tmap_b)).astype(BF16)
    shrink = jnp.exp(top - most.astype(F32))
    total = total * shrink
    total_hi = total.astype(BF16)
    total_lo = (total - total_hi.astype(F32)).astype(BF16)
    high = jnp.where(
        cnt_v[:, 0:64] > 0.0, dot_nt(most, first_b), sum_m.astype(BF16).astype(F32)
    )
    sums = dot_nt(total_hi, tmap_b) + dot_nt(total_lo, tmap_b) + sum_l * jnp.exp(sum_m - high)
    for y in range(4):
        zsend_v[y, :, 0:64] = high[2 * y : 2 * y + 2]
        zsend_v[y, :, 64:128] = sums[2 * y : 2 * y + 2]
    col_m = col_v[0:64, 0:8]
    high_col = jnp.where(
        tmap_v[2][:, 0:8].astype(F32) > 0.0, dot_nt(first_b, most), col_m.astype(BF16).astype(F32)
    )
    factor = jnp.exp(col_m - high_col)
    tmap_f = tmap_b[:, 0:CAP].astype(F32)
    lane8 = iota((64, 8), 1)
    for h in range(8):
        mine = (tmap_f * shrink[h : h + 1, 0:CAP]).astype(BF16)
        a = dot(mine, acc_v[h * STRIDE : h * STRIDE + CAP, :].astype(BF16))
        keep = jnp.sum(jnp.where(lane8 == h, factor, 0.0), axis=1, keepdims=True)
        a = (a + summed_v[h * 64 : h * 64 + 64, :] * keep).astype(BF16)
        for t in range(4):
            send_v[(h // 2) * 4 + t, h % 2] = a[t * 16 : t * 16 + 16]

    with jax.named_scope("barrier"):
        pl.semaphore_wait(barrier, 22)

    def remote(src, dst, send_sem, recv_sem, where):
        return pltpu.make_async_remote_copy(
            src_ref=src, dst_ref=dst, send_sem=send_sem, recv_sem=recv_sem,
            device_id=where, device_id_type=pl.DeviceIdType.MESH,
        )

    order = sorted(shifts, key=lambda d: -(min(d[0], 4 - d[0]) + min(d[1], 4 - d[1])))
    pushes = []
    for dy, dx in order:
        d = dy * 4 + dx
        peer = seq_at(dy, dx)
        for push in (
            remote(zsend_v.at[peer // 4], zrecv_v.at[d], rz_s.at[d], rz_r.at[d], {"seq": peer}),
            remote(send_v.at[peer], recv_v.at[d], rs_s.at[d], rs_r.at[d], {"seq": peer}),
        ):
            push.start()
            pushes.append(push)
    recv_v[0] = send_v[seq]
    zrecv_v[0] = zsend_v[sy]
    with jax.named_scope("rs_recv"):
        for push in pushes:
            push.wait_recv()
    pick = where_true(iota((16, 128), 1) == iota((16, 128), 0) + 16 * sx)
    heads = []
    for e in range(2):
        z = jnp.concatenate([zrecv_v[d, e : e + 1, :] for d in range(16)], axis=0)
        f = jnp.exp(z - jnp.max(z, axis=0, keepdims=True))
        f = jnp.where(iota((16, 128), 1) < 64, f, 0.0)
        whole = jnp.sum(f * pltpu.roll(z, 64, 1), axis=0, keepdims=True)
        g = jnp.where(iota((16, 128), 1) < 64, f / whole, 0.0)
        g_hi = g.astype(BF16)
        g_lo = (g - g_hi.astype(F32)).astype(BF16)
        share = dot_nt(pick, g_hi) + dot_nt(pick, g_lo)
        found = jnp.zeros((16, 128), F32)
        for d in range(16):
            part = jnp.where(iota((16, 16), 1) == d, share, 0.0)
            found = found + recv_v[d, e].astype(F32) * jnp.sum(part, axis=1, keepdims=True)
        piece_v[e] = found.astype(BF16)

    def place(o):
        return att_v.at[pl.ds(2 * (o // 4), 2), pl.ds(pl.multiple_of(16 * (o % 4), 16), 16), :]

    spreads = {}
    for dy, dx in order:
        d = dy * 4 + dx
        peer = seq_at(dy, dx)
        spreads[dy, dx] = remote(piece_v, place(seq), ag_s.at[d], ag_r.at[d], {"seq": peer})
        spreads[dy, dx].start()
    place(seq)[...] = piece_v[...]
    for push in pushes:
        push.wait_send()
    l_w.wait()

    terms = None
    for dy in (0, 1, 3, 2):
        with jax.named_scope(f"ag_recv{dy}"):
            for dx in range(4):
                if dy or dx:
                    d = dy * 4 + dx
                    source = seq_at(-dy, -dx)
                    remote(
                        piece_v, place(source), ag_s.at[d], ag_r.at[d], {"seq": source}
                    ).wait_recv()
        y = lax.rem(sy - dy + 4, 4)
        for e in range(2):
            term = dot(att_v[2 * y + e], w_v[2 * y + e])
            terms = term if terms is None else terms + term
    for e in range(8):
        psend_v[e] = terms[e * 8 : e * 8 + 8, :].astype(BF16)
    hands = []
    for e in (4, 5, 3, 6, 2, 7, 1):
        peer = lax.rem(kvh + e, 8)
        hand = remote(psend_v.at[peer], precv_v.at[e], pj_s.at[e], pj_r.at[e], {"kvh": peer})
        hand.start()
        hands.append(hand)
    for spread in spreads.values():
        spread.wait_send()
    result = psend_v[kvh].astype(F32)
    with jax.named_scope("pj_recv"):
        for hand in hands:
            hand.wait_recv()
    for e in range(1, 8):
        result = result + precv_v[e].astype(F32)
    out_ref[...] = result.astype(BF16)
    with jax.named_scope("pj_send"):
        for hand in hands:
            hand.wait_send()


def on_device(queries, keys, values, rep_keys, rep_values, block_ids, block_counts, out_weight):
    vmem, smem, dma = pltpu.VMEM, pltpu.SMEM, pltpu.SemaphoreType.DMA
    any_spec = pl.BlockSpec(memory_space=pltpu.HBM)
    return pl.pallas_call(
        kernel,
        out_shape=jax.ShapeDtypeStruct((8, 512), BF16),
        in_specs=[any_spec] * 8,
        out_specs=pl.BlockSpec(memory_space=pltpu.VMEM),
        scratch_shapes=[
            vmem((64, 8, 128), BF16), vmem((128, 128, 128), BF16), vmem((128, 128, 128), BF16),
            vmem((512, 128), BF16), vmem((512, 128), BF16), vmem((16, 64), jnp.int32),
            vmem((8, 128, 512), BF16), smem((128,), jnp.int32), vmem((16, 128), jnp.int32),
            smem((16, 128), jnp.int32),
            vmem((16, 128), F32), vmem((64, 8, 128), F32), vmem((520, 128), F32),
            vmem((512, 128), BF16), vmem((512, 512), F32), vmem((512, 512), BF16), vmem((CAP // 4, 32, 256), BF16),
            vmem((9 * STRIDE, 128), F32), vmem((512, 128), F32), vmem((8, 256), F32),
            vmem((3, 64, 256), BF16), vmem((128, 128), F32), vmem((16, 128), F32),
            vmem((8, 128), F32),
            vmem((16, 2, 16, 128), BF16), vmem((16, 2, 16, 128), BF16),
            vmem((4, 2, 128), F32), vmem((16, 2, 128), F32), vmem((2, 16, 128), BF16),
            vmem((8, 64, 128), BF16), vmem((8, 8, 512), BF16), vmem((8, 8, 512), BF16),
            dma((8,)), dma, dma((16,)), dma((16,)), dma((16,)), dma((16,)), dma((16,)), dma((16,)),
            dma((8,)), dma((8,)),
        ],
        compiler_params=pltpu.CompilerParams(collective_id=0, has_side_effects=True, vmem_limit_bytes=24 * 1024 * 1024),
        name="decode",
    )(*[pltpu.with_memory_space_constraint(x, pltpu.HBM) for x in (
        queries,
        keys.reshape(keys.shape[0], keys.shape[2], keys.shape[3]),
        values.reshape(values.shape[0], values.shape[2], values.shape[3]),
        rep_keys.reshape(-1, rep_keys.shape[3]),
        rep_values.reshape(-1, rep_values.shape[3]),
        jnp.transpose(block_ids, (1, 2, 0)).reshape(block_ids.shape[2], block_ids.shape[0]),
        block_counts,
        out_weight.reshape(8, 128, out_weight.shape[1]),
    )])


def solution(mesh):
    in_specs = (
        P(None, "kvh", None),
        P("seq", "kvh", None, None),
        P("seq", "kvh", None, None),
        P("seq", "kvh", None, None),
        P("seq", "kvh", None, None),
        P(None, "kvh", None),
        P("seq"),
        P("kvh", "seq"),
    )
    return jax.shard_map(
        on_device, mesh=mesh, in_specs=in_specs, out_specs=P("kvh", "seq"), check_vma=False
    )
```

```python
import functools
import math

import jax
import jax.numpy as jnp
from jax import lax
from jax.experimental import pallas as pl
from jax.experimental.pallas import tpu as pltpu
from jax.sharding import PartitionSpec as P

CAP = 192
STRIDE = 196
FLOOR = -1e30
F32 = jnp.float32
BF16 = jnp.bfloat16
NT = (((1,), (1,)), ((), ()))


def dot(a, b):
    return jnp.dot(a, b, preferred_element_type=F32)


def dot_nt(a, b):
    return lax.dot_general(a, b, NT, preferred_element_type=F32)


def iota(shape, dim):
    return lax.broadcasted_iota(jnp.int32, shape, dim)


def kernel(
    q_hbm, k_hbm, v_hbm, rk_hbm, rv_hbm, ids_hbm, cnt_hbm, w_hbm,
    out_ref,
    small_v, k_v, v_v, ids_v, w_v, cnt_s, slot_v, slot_s,
    wide_v, q3, q32, qh_v, rs_v, rp_v, weight_v, acc_v, summed_v, seg_v,
    tmap_v, col_v, row_v, cnt_v, send_v, recv_v, zsend_v, zrecv_v, piece_v, att_v, psend_v, precv_v,
    in_sem, slot_sem, rs_s, rs_r, rz_s, rz_r, ag_s, ag_r, pj_s, pj_r,
):
    seq = lax.axis_index("seq")
    kvh = lax.axis_index("kvh")
    sy, sx = seq // 4, seq % 4
    scale = 1.0 / math.sqrt(128)

    def seq_at(dy, dx):
        return lax.rem(sy + dy + 4, 4) * 4 + lax.rem(sx + dx + 4, 4)

    shifts = [(dy, dx) for dy in range(4) for dx in range(4) if dy or dx]

    barrier = pltpu.get_barrier_semaphore()
    loads = [
        pltpu.make_async_copy(src, dst, in_sem.at[i])
        for src, dst, i in [
            (ids_hbm, ids_v, 0), (cnt_hbm, cnt_s, 1), (q_hbm, small_v.at[0], 2),
            (rk_hbm, small_v.at[1], 2), (rv_hbm, small_v.at[2], 2), (k_hbm, k_v, 3),
            (v_hbm, v_v, 4), (w_hbm, w_v, 5),
        ]
    ]
    for load in loads:
        load.start()
    l_ids, l_cnt, _, _, _, l_k, l_v, l_w = loads

    def wait_for(like, sem):
        pltpu.make_async_copy(like, like, sem).wait()

    for dy, dx in shifts:
        pl.semaphore_signal(
            barrier, inc=1, device_id={"seq": seq_at(dy, dx)}, device_id_type=pl.DeviceIdType.MESH
        )
    for e in range(1, 8):
        pl.semaphore_signal(
            barrier, inc=1, device_id={"kvh": lax.rem(kvh + e, 8)}, device_id_type=pl.DeviceIdType.MESH
        )

    def where_true(cond):
        return jnp.where(cond, 1.0, 0.0).astype(BF16)

    wide_v[...] = jnp.full_like(wide_v, -1.0)
    col_v[...] = jnp.zeros_like(col_v)
    slot_v[...] = jnp.zeros_like(slot_v)
    with jax.named_scope("wait_ids"):
        l_ids.wait()
    wide_v[:, 0:64] = ids_v[...].astype(F32)
    ids = wide_v[...]
    first_id = (seq * 128).astype(F32)
    local = (ids >= first_id) & (ids < first_id + 128.0)
    block = ids - first_id
    hit = where_true(local)
    before = where_true(iota((16, 16), 1) < iota((16, 16), 0))
    counts = dot(jnp.ones((256, 16), BF16), hit)
    earlier = where_true(iota((128, 128), 0) < iota((128, 128), 1))
    rank = dot(counts[0:16].astype(BF16), earlier) + dot(before, hit)
    rank = jnp.where(local, rank, -1.0).astype(jnp.int32)
    high, low = rank >> 4, rank & 15
    digit = iota((16, 128), 0)
    token_at = iota((16, 128), 1).astype(F32)
    blocks, tokens, lows = [], [], []
    for s in range(16):
        same = high[s : s + 1, :] == digit
        blocks.append(jnp.where(same, block[s : s + 1, :], 0.0))
        tokens.append(jnp.where(same, token_at, 0.0))
        lows.append(jnp.where(low[s : s + 1, :] == digit, 1.0, 0.0))
    chosen = [jnp.concatenate(x, axis=1).astype(BF16) for x in (blocks, tokens, lows)]
    slots = dot_nt(chosen[2], jnp.concatenate(chosen[0:2], axis=0)).astype(jnp.int32)
    slot_v[:, 0:32] = slots & jnp.where(iota((16, 32), 1) < 16, 127, 63)
    to_smem = pltpu.make_async_copy(slot_v, slot_s, slot_sem)
    to_smem.start()
    cnt_v[...] = counts[0:8]
    counts = counts.astype(BF16)
    base = dot_nt(where_true(iota((64, 128), 1) < iota((64, 128), 0)), counts)
    count = dot_nt(where_true(iota((64, 128), 1) == iota((64, 128), 0)), counts)
    at = iota((64, 256), 1).astype(F32)
    tmap = jnp.where((at >= base) & (at < base + count), 1.0, 0.0)
    slot_token = jnp.sum(tmap * (iota((64, 256), 0) + 1).astype(F32), axis=0, keepdims=True)
    seg_v[...] = jnp.broadcast_to(slot_token, (8, 256))
    tmap_v[0] = tmap.astype(BF16)
    tmap_v[1] = where_true((at == base) & (count > 0.0))
    tmap_v[2] = where_true(count > 0.0)

    with jax.named_scope("wait_q"):
        wait_for(small_v, in_sem.at[2])
    wide = small_v[0].astype(F32)
    q3[...] = wide.reshape(64, 8, 128)
    q32[0:512, :] = wide
    for h in range(8):
        qh_v[h * 64 : h * 64 + 64, :] = q32[pl.ds(h, 64, stride=8), :].astype(BF16)
    rs_v[...] = dot_nt(qh_v[...], small_v[1])
    for h in range(8):
        s = rs_v[h * 64 : h * 64 + 64, :] * scale
        m = jnp.max(s, axis=1, keepdims=True)
        p = jnp.exp(s - m)
        rp_v[h * 64 : h * 64 + 64, :] = p.astype(BF16)
        col_v[0:64, h : h + 1] = m
        col_v[0:64, 8 + h : 9 + h] = jnp.sum(p, axis=1, keepdims=True)
    summed_v[...] = dot(rp_v[...], small_v[2])
    row_v[...] = col_v[...].T[0:16, :]

    lane = iota((8, 128), 1)
    empty = jnp.zeros((8, 128), F32)

    def beside(a, b):
        return jnp.concatenate([a, b], axis=1)

    def four(a, b, c, d):
        rows = [beside(a, empty), beside(empty, b), beside(c, empty), beside(empty, d)]
        return jnp.concatenate(rows, axis=0).astype(BF16)

    def apart(r):
        return r[0:8, 0:128], r[8:16, 0:128], r[16:24, 128:256], r[24:32, 128:256]

    with jax.named_scope("wait_smem"):
        l_cnt.wait()
        to_smem.wait()
    with jax.named_scope("wait_k"):
        l_k.wait()
    tops, totals = [empty, empty], [empty, empty]
    for j in range(0, CAP, 4):
        own = range(4)
        half = j // 128
        blk = [slot_s[j % 16 + i, j // 16] for i in own]
        query = [q3[slot_s[j % 16 + i, 16 + j // 16]] for i in own]
        tile = [k_v[blk[i]] for i in own]
        tile = jnp.concatenate([beside(tile[0], tile[1]), beside(tile[2], tile[3])], axis=0)
        found = apart(dot_nt(four(*query), tile))
        ps = []
        for i in own:
            here = lane == (j + i) % 128
            s = jnp.where(lane < cnt_s[blk[i]], found[i] * scale, FLOOR)
            m = jnp.max(s, axis=1, keepdims=True)
            p = jnp.exp(s - m)
            tops[half] = jnp.where(here, m, tops[half])
            totals[half] = jnp.where(here, jnp.sum(p, axis=1, keepdims=True), totals[half])
            ps.append(p)
        weight_v[j // 4] = four(*ps)
    with jax.named_scope("wait_v"):
        l_v.wait()
    for j in range(0, CAP, 4):
        tile = [v_v[slot_s[j % 16 + i, j // 16]] for i in own]
        tile = jnp.concatenate([beside(tile[0], tile[2]), beside(tile[1], tile[3])], axis=0)
        found = apart(dot(weight_v[j // 4], tile))
        for i in own:
            acc_v[pl.ds(j + i, 8, stride=STRIDE), :] = found[i]

    top, total = beside(*tops), beside(*totals)
    token = seg_v[...]
    most = top
    for back in (False, True):
        for k in (1, 2, 4, 8):
            by = 256 - k if back else k
            same = pltpu.roll(token, by, 1) == token
            most = jnp.maximum(most, jnp.where(same, pltpu.roll(most, by, 1), FLOOR))
    tmap_b, first_b = tmap_v[0], tmap_v[1]
    sum_m, sum_l = row_v[0:8, 0:64], row_v[8:16, 0:64]
    most = jnp.maximum(most, dot(sum_m.astype(BF16), tmap_b)).astype(BF16)
    shrink = jnp.exp(top - most.astype(F32))
    total = total * shrink
    total_hi = total.astype(BF16)
    total_lo = (total - total_hi.astype(F32)).astype(BF16)
    high = jnp.where(
        cnt_v[:, 0:64] > 0.0, dot_nt(most, first_b), sum_m.astype(BF16).astype(F32)
    )
    sums = dot_nt(total_hi, tmap_b) + dot_nt(total_lo, tmap_b) + sum_l * jnp.exp(sum_m - high)
    for y in range(4):
        zsend_v[y, :, 0:64] = high[2 * y : 2 * y + 2]
        zsend_v[y, :, 64:128] = sums[2 * y : 2 * y + 2]
    col_m = col_v[0:64, 0:8]
    high_col = jnp.where(
        tmap_v[2][:, 0:8].astype(F32) > 0.0, dot_nt(first_b, most), col_m.astype(BF16).astype(F32)
    )
    factor = jnp.exp(col_m - high_col)
    tmap_f = tmap_b[:, 0:CAP].astype(F32)
    lane8 = iota((64, 8), 1)
    for h in range(8):
        mine = (tmap_f * shrink[h : h + 1, 0:CAP]).astype(BF16)
        a = dot(mine, acc_v[h * STRIDE : h * STRIDE + CAP, :].astype(BF16))
        keep = jnp.sum(jnp.where(lane8 == h, factor, 0.0), axis=1, keepdims=True)
        a = (a + summed_v[h * 64 : h * 64 + 64, :] * keep).astype(BF16)
        for t in range(4):
            send_v[(h // 2) * 4 + t, h % 2] = a[t * 16 : t * 16 + 16]

    with jax.named_scope("barrier"):
        pl.semaphore_wait(barrier, 22)

    def remote(src, dst, send_sem, recv_sem, where):
        return pltpu.make_async_remote_copy(
            src_ref=src, dst_ref=dst, send_sem=send_sem, recv_sem=recv_sem,
            device_id=where, device_id_type=pl.DeviceIdType.MESH,
        )

    order = sorted(shifts, key=lambda d: -(min(d[0], 4 - d[0]) + min(d[1], 4 - d[1])))
    for dy, dx in order:
        d = dy * 4 + dx
        peer = seq_at(dy, dx)
        for push in (
            remote(zsend_v.at[peer // 4], zrecv_v.at[d], rz_s, rz_r, {"seq": peer}),
            remote(send_v.at[peer], recv_v.at[d], rs_s, rs_r, {"seq": peer}),
        ):
            push.start()
    recv_v[0] = send_v[seq]
    zrecv_v[0] = zsend_v[sy]
    with jax.named_scope("rs_recv"):
        wait_for(zrecv_v.at[pl.ds(1, 15)], rz_r)
        wait_for(recv_v.at[pl.ds(1, 15)], rs_r)
    pick = where_true(iota((16, 128), 1) == iota((16, 128), 0) + 16 * sx)
    heads = []
    for e in range(2):
        z = jnp.concatenate([zrecv_v[d, e : e + 1, :] for d in range(16)], axis=0)
        f = jnp.exp(z - jnp.max(z, axis=0, keepdims=True))
        f = jnp.where(iota((16, 128), 1) < 64, f, 0.0)
        whole = jnp.sum(f * pltpu.roll(z, 64, 1), axis=0, keepdims=True)
        g = jnp.where(iota((16, 128), 1) < 64, f / whole, 0.0)
        g_hi = g.astype(BF16)
        g_lo = (g - g_hi.astype(F32)).astype(BF16)
        share = dot_nt(pick, g_hi) + dot_nt(pick, g_lo)
        found = jnp.zeros((16, 128), F32)
        for d in range(16):
            part = jnp.where(iota((16, 16), 1) == d, share, 0.0)
            found = found + recv_v[d, e].astype(F32) * jnp.sum(part, axis=1, keepdims=True)
        piece_v[e] = found.astype(BF16)

    def place(o):
        return att_v.at[pl.ds(2 * (o // 4), 2), pl.ds(pl.multiple_of(16 * (o % 4), 16), 16), :]

    for dy, dx in order:
        remote(piece_v, place(seq), ag_s, ag_r.at[dy], {"seq": seq_at(dy, dx)}).start()
    place(seq)[...] = piece_v[...]
    wait_for(zrecv_v.at[pl.ds(1, 15)], rz_s)
    wait_for(send_v.at[pl.ds(1, 15)], rs_s)
    l_w.wait()

    terms = None
    for dy in (0, 1, 3, 2):
        y = lax.rem(sy - dy + 4, 4)
        with jax.named_scope(f"ag_recv{dy}"):
            wait_for(att_v.at[pl.ds(2 * y, 2), pl.ds(0, 64 if dy else 48)], ag_r.at[dy])
        for e in range(2):
            term = dot(att_v[2 * y + e], w_v[2 * y + e])
            terms = term if terms is None else terms + term
    for e in range(8):
        psend_v[e] = terms[e * 8 : e * 8 + 8, :].astype(BF16)
    for e in (4, 5, 3, 6, 2, 7, 1):
        peer = lax.rem(kvh + e, 8)
        remote(psend_v.at[peer], precv_v.at[e], pj_s, pj_r, {"kvh": peer}).start()
    wait_for(recv_v.at[pl.ds(1, 15)], ag_s)
    result = psend_v[kvh].astype(F32)
    with jax.named_scope("pj_recv"):
        wait_for(precv_v.at[pl.ds(1, 7)], pj_r)
    for e in range(1, 8):
        result = result + precv_v[e].astype(F32)
    out_ref[...] = result.astype(BF16)
    with jax.named_scope("pj_send"):
        wait_for(psend_v.at[pl.ds(1, 7)], pj_s)


def on_device(queries, keys, values, rep_keys, rep_values, block_ids, block_counts, out_weight):
    vmem, smem, dma = pltpu.VMEM, pltpu.SMEM, pltpu.SemaphoreType.DMA
    any_spec = pl.BlockSpec(memory_space=pltpu.HBM)
    return pl.pallas_call(
        kernel,
        out_shape=jax.ShapeDtypeStruct((8, 512), BF16),
        in_specs=[any_spec] * 8,
        out_specs=pl.BlockSpec(memory_space=pltpu.VMEM),
        scratch_shapes=[
            vmem((3, 512, 128), BF16), vmem((128, 128, 128), BF16), vmem((128, 128, 128), BF16),
            vmem((16, 64), jnp.int32),
            vmem((8, 128, 512), BF16), smem((128,), jnp.int32), vmem((16, 128), jnp.int32),
            smem((16, 128), jnp.int32),
            vmem((16, 128), F32), vmem((64, 8, 128), F32), vmem((520, 128), F32),
            vmem((512, 128), BF16), vmem((512, 512), F32), vmem((512, 512), BF16), vmem((CAP // 4, 32, 256), BF16),
            vmem((9 * STRIDE, 128), F32), vmem((512, 128), F32), vmem((8, 256), F32),
            vmem((3, 64, 256), BF16), vmem((128, 128), F32), vmem((16, 128), F32),
            vmem((8, 128), F32),
            vmem((16, 2, 16, 128), BF16), vmem((16, 2, 16, 128), BF16),
            vmem((4, 2, 128), F32), vmem((16, 2, 128), F32), vmem((2, 16, 128), BF16),
            vmem((8, 64, 128), BF16), vmem((8, 8, 512), BF16), vmem((8, 8, 512), BF16),
            dma((6,)), dma, dma, dma, dma, dma, dma, dma((4,)), dma, dma,
        ],
        compiler_params=pltpu.CompilerParams(collective_id=0, has_side_effects=True, vmem_limit_bytes=24 * 1024 * 1024),
        name="decode",
    )(*[pltpu.with_memory_space_constraint(x, pltpu.HBM) for x in (
        queries.reshape(-1, queries.shape[2]),
        keys.reshape(keys.shape[0], keys.shape[2], keys.shape[3]),
        values.reshape(values.shape[0], values.shape[2], values.shape[3]),
        rep_keys.reshape(-1, rep_keys.shape[3]),
        rep_values.reshape(-1, rep_values.shape[3]),
        jnp.transpose(block_ids, (1, 2, 0)).reshape(block_ids.shape[2], block_ids.shape[0]),
        block_counts,
        out_weight.reshape(8, 128, out_weight.shape[1]),
    )])


def solution(mesh):
    in_specs = (
        P(None, "kvh", None),
        P("seq", "kvh", None, None),
        P("seq", "kvh", None, None),
        P("seq", "kvh", None, None),
        P("seq", "kvh", None, None),
        P(None, "kvh", None),
        P("seq"),
        P("kvh", "seq"),
    )
    return jax.shard_map(
        on_device, mesh=mesh, in_specs=in_specs, out_specs=P("kvh", "seq"), check_vma=False
    )
```

```python
import functools
import math

import jax
import jax.numpy as jnp
from jax import lax
from jax.experimental import pallas as pl
from jax.experimental.pallas import tpu as pltpu
from jax.sharding import PartitionSpec as P

CAP = 192
STRIDE = 196
FLOOR = -1e30
F32 = jnp.float32
BF16 = jnp.bfloat16
NT = (((1,), (1,)), ((), ()))


def dot(a, b):
    return jnp.dot(a, b, preferred_element_type=F32)


def dot_nt(a, b):
    return lax.dot_general(a, b, NT, preferred_element_type=F32)


def iota(shape, dim):
    return lax.broadcasted_iota(jnp.int32, shape, dim)


def kernel(
    q_hbm, k_hbm, v_hbm, rk_hbm, rv_hbm, ids_hbm, cnt_hbm, w_hbm,
    out_ref,
    small_v, k_v, v_v, ids_v, w_v, cnt_s, slot_v, slot_s,
    wide_v, q3, q32, qh_v, rs_v, rp_v, weight_v, acc_v, summed_v, seg_v,
    tmap_v, col_v, row_v, cnt_v, send_v, recv_v, zsend_v, zrecv_v, piece_v, att_v, psend_v, precv_v,
    in_sem, slot_sem, rs_s, rs_r, rz_s, rz_r, ag_s, ag_r, pj_s, pj_r,
):
    seq = lax.axis_index("seq")
    kvh = lax.axis_index("kvh")
    sy, sx = seq // 4, seq % 4
    core = lax.rem(kvh, 2)
    other = kvh + 1 - 2 * core
    keeper = kvh + 1 - core
    scale = 1.0 / math.sqrt(128)

    def seq_at(dy, dx):
        return lax.rem(sy + dy + 4, 4) * 4 + lax.rem(sx + dx + 4, 4)

    shifts = [(dy, dx) for dy in range(4) for dx in range(4) if dy or dx]

    barrier = pltpu.get_barrier_semaphore()
    loads = [
        pltpu.make_async_copy(src, dst, in_sem.at[i])
        for src, dst, i in [
            (ids_hbm, ids_v, 0), (cnt_hbm, cnt_s, 1), (q_hbm, small_v.at[0], 2),
            (rk_hbm, small_v.at[1], 2), (rv_hbm, small_v.at[2], 2), (k_hbm, k_v, 3),
            (v_hbm, v_v, 4), (w_hbm, w_v, 5),
        ]
    ]
    for load in loads:
        load.start()
    l_ids, l_cnt, _, _, _, l_k, l_v, l_w = loads

    def wait_for(like, sem):
        pltpu.make_async_copy(like, like, sem).wait()

    for dy, dx in shifts:
        pl.semaphore_signal(
            barrier, inc=1, device_id={"seq": seq_at(dy, dx)}, device_id_type=pl.DeviceIdType.MESH
        )
        pl.semaphore_signal(
            barrier,
            inc=1,
            device_id={"seq": seq_at(dy, dx), "kvh": other},
            device_id_type=pl.DeviceIdType.MESH,
        )
    for e in range(1, 8):
        pl.semaphore_signal(
            barrier, inc=1, device_id={"kvh": lax.rem(kvh + e, 8)}, device_id_type=pl.DeviceIdType.MESH
        )

    def where_true(cond):
        return jnp.where(cond, 1.0, 0.0).astype(BF16)

    wide_v[...] = jnp.full_like(wide_v, -1.0)
    col_v[...] = jnp.zeros_like(col_v)
    slot_v[...] = jnp.zeros_like(slot_v)
    with jax.named_scope("wait_ids"):
        l_ids.wait()
    wide_v[:, 0:64] = ids_v[...].astype(F32)
    ids = wide_v[...]
    first_id = (seq * 128).astype(F32)
    local = (ids >= first_id) & (ids < first_id + 128.0)
    block = ids - first_id
    hit = where_true(local)
    before = where_true(iota((16, 16), 1) < iota((16, 16), 0))
    counts = dot(jnp.ones((256, 16), BF16), hit)
    earlier = where_true(iota((128, 128), 0) < iota((128, 128), 1))
    rank = dot(counts[0:16].astype(BF16), earlier) + dot(before, hit)
    rank = jnp.where(local, rank, -1.0).astype(jnp.int32)
    high, low = rank >> 4, rank & 15
    digit = iota((16, 128), 0)
    token_at = iota((16, 128), 1).astype(F32)
    blocks, tokens, lows = [], [], []
    for s in range(16):
        same = high[s : s + 1, :] == digit
        blocks.append(jnp.where(same, block[s : s + 1, :], 0.0))
        tokens.append(jnp.where(same, token_at, 0.0))
        lows.append(jnp.where(low[s : s + 1, :] == digit, 1.0, 0.0))
    chosen = [jnp.concatenate(x, axis=1).astype(BF16) for x in (blocks, tokens, lows)]
    slots = dot_nt(chosen[2], jnp.concatenate(chosen[0:2], axis=0)).astype(jnp.int32)
    slot_v[:, 0:32] = slots & jnp.where(iota((16, 32), 1) < 16, 127, 63)
    to_smem = pltpu.make_async_copy(slot_v, slot_s, slot_sem)
    to_smem.start()
    cnt_v[...] = counts[0:8]
    counts = counts.astype(BF16)
    base = dot_nt(where_true(iota((64, 128), 1) < iota((64, 128), 0)), counts)
    count = dot_nt(where_true(iota((64, 128), 1) == iota((64, 128), 0)), counts)
    at = iota((64, 256), 1).astype(F32)
    tmap = jnp.where((at >= base) & (at < base + count), 1.0, 0.0)
    slot_token = jnp.sum(tmap * (iota((64, 256), 0) + 1).astype(F32), axis=0, keepdims=True)
    seg_v[...] = jnp.broadcast_to(slot_token, (8, 256))
    tmap_v[0] = tmap.astype(BF16)
    tmap_v[1] = where_true((at == base) & (count > 0.0))
    tmap_v[2] = where_true(count > 0.0)

    with jax.named_scope("wait_q"):
        wait_for(small_v, in_sem.at[2])
    wide = small_v[0].astype(F32)
    q3[...] = wide.reshape(64, 8, 128)
    q32[0:512, :] = wide
    for h in range(8):
        qh_v[h * 64 : h * 64 + 64, :] = q32[pl.ds(h, 64, stride=8), :].astype(BF16)
    rs_v[...] = dot_nt(qh_v[...], small_v[1])
    for h in range(8):
        s = rs_v[h * 64 : h * 64 + 64, :] * scale
        m = jnp.max(s, axis=1, keepdims=True)
        p = jnp.exp(s - m)
        rp_v[h * 64 : h * 64 + 64, :] = p.astype(BF16)
        col_v[0:64, h : h + 1] = m
        col_v[0:64, 8 + h : 9 + h] = jnp.sum(p, axis=1, keepdims=True)
    summed_v[...] = dot(rp_v[...], small_v[2])
    row_v[...] = col_v[...].T[0:16, :]

    lane = iota((8, 128), 1)
    empty = jnp.zeros((8, 128), F32)

    def beside(a, b):
        return jnp.concatenate([a, b], axis=1)

    def four(a, b, c, d):
        rows = [beside(a, empty), beside(empty, b), beside(c, empty), beside(empty, d)]
        return jnp.concatenate(rows, axis=0).astype(BF16)

    def apart(r):
        return r[0:8, 0:128], r[8:16, 0:128], r[16:24, 128:256], r[24:32, 128:256]

    with jax.named_scope("wait_smem"):
        l_cnt.wait()
        to_smem.wait()
    with jax.named_scope("wait_k"):
        l_k.wait()
    tops, totals = [empty, empty], [empty, empty]
    for j in range(0, CAP, 4):
        own = range(4)
        half = j // 128
        blk = [slot_s[j % 16 + i, j // 16] for i in own]
        query = [q3[slot_s[j % 16 + i, 16 + j // 16]] for i in own]
        tile = [k_v[blk[i]] for i in own]
        tile = jnp.concatenate([beside(tile[0], tile[1]), beside(tile[2], tile[3])], axis=0)
        found = apart(dot_nt(four(*query), tile))
        ps = []
        for i in own:
            here = lane == (j + i) % 128
            s = jnp.where(lane < cnt_s[blk[i]], found[i] * scale, FLOOR)
            m = jnp.max(s, axis=1, keepdims=True)
            p = jnp.exp(s - m)
            tops[half] = jnp.where(here, m, tops[half])
            totals[half] = jnp.where(here, jnp.sum(p, axis=1, keepdims=True), totals[half])
            ps.append(p)
        weight_v[j // 4] = four(*ps)
    with jax.named_scope("wait_v"):
        l_v.wait()
    for j in range(0, CAP, 4):
        tile = [v_v[slot_s[j % 16 + i, j // 16]] for i in own]
        tile = jnp.concatenate([beside(tile[0], tile[2]), beside(tile[1], tile[3])], axis=0)
        found = apart(dot(weight_v[j // 4], tile))
        for i in own:
            acc_v[pl.ds(j + i, 8, stride=STRIDE), :] = found[i]

    top, total = beside(*tops), beside(*totals)
    token = seg_v[...]
    most = top
    for back in (False, True):
        for k in (1, 2, 4, 8):
            by = 256 - k if back else k
            same = pltpu.roll(token, by, 1) == token
            most = jnp.maximum(most, jnp.where(same, pltpu.roll(most, by, 1), FLOOR))
    tmap_b, first_b = tmap_v[0], tmap_v[1]
    sum_m, sum_l = row_v[0:8, 0:64], row_v[8:16, 0:64]
    most = jnp.maximum(most, dot(sum_m.astype(BF16), tmap_b)).astype(BF16)
    shrink = jnp.exp(top - most.astype(F32))
    total = total * shrink
    total_hi = total.astype(BF16)
    total_lo = (total - total_hi.astype(F32)).astype(BF16)
    high = jnp.where(
        cnt_v[:, 0:64] > 0.0, dot_nt(most, first_b), sum_m.astype(BF16).astype(F32)
    )
    sums = dot_nt(total_hi, tmap_b) + dot_nt(total_lo, tmap_b) + sum_l * jnp.exp(sum_m - high)
    for y in range(4):
        zsend_v[y, :, 0:64] = high[2 * y : 2 * y + 2]
        zsend_v[y, :, 64:128] = sums[2 * y : 2 * y + 2]
    col_m = col_v[0:64, 0:8]
    high_col = jnp.where(
        tmap_v[2][:, 0:8].astype(F32) > 0.0, dot_nt(first_b, most), col_m.astype(BF16).astype(F32)
    )
    factor = jnp.exp(col_m - high_col)
    tmap_f = tmap_b[:, 0:CAP].astype(F32)
    lane8 = iota((64, 8), 1)
    for h in range(8):
        mine = (tmap_f * shrink[h : h + 1, 0:CAP]).astype(BF16)
        a = dot(mine, acc_v[h * STRIDE : h * STRIDE + CAP, :].astype(BF16))
        keep = jnp.sum(jnp.where(lane8 == h, factor, 0.0), axis=1, keepdims=True)
        a = (a + summed_v[h * 64 : h * 64 + 64, :] * keep).astype(BF16)
        for t in range(4):
            send_v[(h // 2) * 4 + t, h % 2] = a[t * 16 : t * 16 + 16]

    with jax.named_scope("barrier"):
        pl.semaphore_wait(barrier, 37)

    def remote(src, dst, send_sem, recv_sem, where):
        return pltpu.make_async_remote_copy(
            src_ref=src, dst_ref=dst, send_sem=send_sem, recv_sem=recv_sem,
            device_id=where, device_id_type=pl.DeviceIdType.MESH,
        )

    order = sorted(shifts, key=lambda d: -(min(d[0], 4 - d[0]) + min(d[1], 4 - d[1])))

    def give(dy, dx):
        d = dy * 4 + dx
        peer = seq_at(dy, dx)
        at = {"seq": peer, "kvh": keeper}
        remote(
            zsend_v.at[peer // 4], zrecv_v.at[core, d], rz_s, rz_r.at[core], at
        ).start()
        remote(send_v.at[peer], recv_v.at[core, d], rs_s, rs_r.at[core], at).start()

    for dy, dx in order:
        give(dy, dx)

    @pl.when(core == 0)
    def _():
        give(0, 0)

    def place(o):
        return att_v.at[pl.ds(2 * (o // 4), 2), pl.ds(pl.multiple_of(16 * (o % 4), 16), 16), :]

    def combined(group):
        heads = []
        for e in range(2):
            z = jnp.concatenate([zrecv_v[group, d, e : e + 1, :] for d in range(16)], axis=0)
            f = jnp.exp(z - jnp.max(z, axis=0, keepdims=True))
            f = jnp.where(iota((16, 128), 1) < 64, f, 0.0)
            whole = jnp.sum(f * pltpu.roll(z, 64, 1), axis=0, keepdims=True)
            g = jnp.where(iota((16, 128), 1) < 64, f / whole, 0.0)
            g_hi = g.astype(BF16)
            g_lo = (g - g_hi.astype(F32)).astype(BF16)
            share = dot_nt(pick, g_hi) + dot_nt(pick, g_lo)
            found = jnp.zeros((16, 128), F32)
            for d in range(16):
                part = jnp.where(iota((16, 16), 1) == d, share, 0.0)
                found = found + recv_v[group, d, e].astype(F32) * jnp.sum(
                    part, axis=1, keepdims=True
                )
            piece_v[group, e] = found.astype(BF16)

    pick = where_true(iota((16, 128), 1) == iota((16, 128), 0) + 16 * sx)

    @pl.when(core == 1)
    def _():
        with jax.named_scope("rs_recv0"):
            wait_for(zrecv_v.at[0], rz_r.at[0])
            wait_for(recv_v.at[0], rs_r.at[0])
        combined(0)
        for dy, dx in order + [(0, 0)]:
            at = {"seq": seq_at(dy, dx), "kvh": other}
            remote(piece_v.at[0], place(seq), ag_s.at[0], ag_r.at[dy], at).start()
        recv_v[1, 0] = send_v[seq]
        zrecv_v[1, 0] = zsend_v[sy]
        with jax.named_scope("rs_recv1"):
            wait_for(zrecv_v.at[1, pl.ds(1, 15)], rz_r.at[1])
            wait_for(recv_v.at[1, pl.ds(1, 15)], rs_r.at[1])
        combined(1)
        for dy, dx in order:
            at = {"seq": seq_at(dy, dx)}
            remote(piece_v.at[1], place(seq), ag_s.at[1], ag_r.at[dy], at).start()
        place(seq)[...] = piece_v[1]

    l_w.wait()

    terms = None
    for dy in (0, 1, 3, 2):
        y = lax.rem(sy - dy + 4, 4)
        with jax.named_scope(f"ag_recv{dy}"):
            if dy:
                wait_for(att_v.at[pl.ds(2 * y, 2)], ag_r.at[dy])
            else:

                @pl.when(core == 0)
                def _():
                    wait_for(att_v.at[pl.ds(2 * y, 2)], ag_r.at[0])

                @pl.when(core == 1)
                def _():
                    wait_for(att_v.at[pl.ds(2 * y, 2), pl.ds(0, 48)], ag_r.at[0])

        for e in range(2):
            term = dot(att_v[2 * y + e], w_v[2 * y + e])
            terms = term if terms is None else terms + term
    for e in range(8):
        psend_v[e] = terms[e * 8 : e * 8 + 8, :].astype(BF16)
    for e in (4, 5, 3, 6, 2, 7, 1):
        peer = lax.rem(kvh + e, 8)
        remote(psend_v.at[peer], precv_v.at[e], pj_s, pj_r, {"kvh": peer}).start()

    @pl.when(core == 0)
    def _():
        wait_for(zrecv_v.at[0], rz_s)
        wait_for(recv_v.at[0], rs_s)

    @pl.when(core == 1)
    def _():
        wait_for(zrecv_v.at[1, pl.ds(1, 15)], rz_s)
        wait_for(recv_v.at[1, pl.ds(1, 15)], rs_s)
        wait_for(recv_v.at[0], ag_s.at[0])
        wait_for(recv_v.at[1, pl.ds(1, 15)], ag_s.at[1])

    result = psend_v[kvh].astype(F32)
    with jax.named_scope("pj_recv"):
        wait_for(precv_v.at[pl.ds(1, 7)], pj_r)
    for e in range(1, 8):
        result = result + precv_v[e].astype(F32)
    out_ref[...] = result.astype(BF16)
    with jax.named_scope("pj_send"):
        wait_for(psend_v.at[pl.ds(1, 7)], pj_s)


def on_device(queries, keys, values, rep_keys, rep_values, block_ids, block_counts, out_weight):
    vmem, smem, dma = pltpu.VMEM, pltpu.SMEM, pltpu.SemaphoreType.DMA
    any_spec = pl.BlockSpec(memory_space=pltpu.HBM)
    return pl.pallas_call(
        kernel,
        out_shape=jax.ShapeDtypeStruct((8, 512), BF16),
        in_specs=[any_spec] * 8,
        out_specs=pl.BlockSpec(memory_space=pltpu.VMEM),
        scratch_shapes=[
            vmem((3, 512, 128), BF16), vmem((128, 128, 128), BF16), vmem((128, 128, 128), BF16),
            vmem((16, 64), jnp.int32),
            vmem((8, 128, 512), BF16), smem((128,), jnp.int32), vmem((16, 128), jnp.int32),
            smem((16, 128), jnp.int32),
            vmem((16, 128), F32), vmem((64, 8, 128), F32), vmem((520, 128), F32),
            vmem((512, 128), BF16), vmem((512, 512), F32), vmem((512, 512), BF16), vmem((CAP // 4, 32, 256), BF16),
            vmem((9 * STRIDE, 128), F32), vmem((512, 128), F32), vmem((8, 256), F32),
            vmem((3, 64, 256), BF16), vmem((128, 128), F32), vmem((16, 128), F32),
            vmem((8, 128), F32),
            vmem((16, 2, 16, 128), BF16), vmem((2, 16, 2, 16, 128), BF16),
            vmem((4, 2, 128), F32), vmem((2, 16, 2, 128), F32), vmem((2, 2, 16, 128), BF16),
            vmem((8, 64, 128), BF16), vmem((8, 8, 512), BF16), vmem((8, 8, 512), BF16),
            dma((6,)), dma, dma, dma((2,)), dma, dma((2,)), dma((2,)), dma((4,)), dma, dma,
        ],
        compiler_params=pltpu.CompilerParams(collective_id=0, has_side_effects=True, vmem_limit_bytes=24 * 1024 * 1024),
        name="decode",
    )(*[pltpu.with_memory_space_constraint(x, pltpu.HBM) for x in (
        queries.reshape(-1, queries.shape[2]),
        keys.reshape(keys.shape[0], keys.shape[2], keys.shape[3]),
        values.reshape(values.shape[0], values.shape[2], values.shape[3]),
        rep_keys.reshape(-1, rep_keys.shape[3]),
        rep_values.reshape(-1, rep_values.shape[3]),
        jnp.transpose(block_ids, (1, 2, 0)).reshape(block_ids.shape[2], block_ids.shape[0]),
        block_counts,
        out_weight.reshape(8, 128, out_weight.shape[1]),
    )])


def solution(mesh):
    in_specs = (
        P(None, "kvh", None),
        P("seq", "kvh", None, None),
        P("seq", "kvh", None, None),
        P("seq", "kvh", None, None),
        P("seq", "kvh", None, None),
        P(None, "kvh", None),
        P("seq"),
        P("kvh", "seq"),
    )
    return jax.shard_map(
        on_device, mesh=mesh, in_specs=in_specs, out_specs=P("kvh", "seq"), check_vma=False
    )
```

```python
import functools
import math

import jax
import jax.numpy as jnp
from jax import lax
from jax.experimental import pallas as pl
from jax.experimental.pallas import tpu as pltpu
from jax.sharding import PartitionSpec as P

CAP = 192
STRIDE = 196
FLOOR = -1e30
F32 = jnp.float32
BF16 = jnp.bfloat16
NT = (((1,), (1,)), ((), ()))


def dot(a, b):
    return jnp.dot(a, b, preferred_element_type=F32)


def dot_nt(a, b):
    return lax.dot_general(a, b, NT, preferred_element_type=F32)


def iota(shape, dim):
    return lax.broadcasted_iota(jnp.int32, shape, dim)


def kernel(
    q_hbm, k_hbm, v_hbm, rk_hbm, rv_hbm, ids_hbm, cnt_hbm, w_hbm,
    out_ref,
    small_v, k_v, v_v, ids_v, w_v, cnt_s, slot_v, slot_s,
    wide_v, q3, q32, qh_v, rs_v, rp_v, weight_v, acc_v, summed_v, seg_v,
    tmap_v, col_v, row_v, cnt_v, send_v, recv_v, zsend_v, zrecv_v, piece_v, att_v, psend_v, precv_v,
    in_sem, slot_sem, rs_s, rs_r, rz_s, rz_r, ag_s, ag_r, pj_s, pj_r,
):
    seq = lax.axis_index("seq")
    kvh = lax.axis_index("kvh")
    sy, sx = seq // 4, seq % 4
    core = lax.rem(kvh, 2)
    other = kvh + 1 - 2 * core
    keeper = kvh + 1 - core
    scale = 1.0 / math.sqrt(128)

    def seq_at(dy, dx):
        return lax.rem(sy + dy + 4, 4) * 4 + lax.rem(sx + dx + 4, 4)

    shifts = [(dy, dx) for dy in range(4) for dx in range(4) if dy or dx]

    barrier = pltpu.get_barrier_semaphore()
    loads = [
        pltpu.make_async_copy(src, dst, in_sem.at[i])
        for src, dst, i in [
            (ids_hbm, ids_v, 0), (cnt_hbm, cnt_s, 1), (q_hbm, small_v.at[0], 2),
            (rk_hbm, small_v.at[1], 2), (rv_hbm, small_v.at[2], 2), (k_hbm, k_v, 3),
            (v_hbm, v_v, 4), (w_hbm, w_v, 5),
        ]
    ]
    for load in loads:
        load.start()
    l_ids, l_cnt, _, _, _, l_k, l_v, l_w = loads

    def wait_for(like, sem):
        pltpu.make_async_copy(like, like, sem).wait()

    for dy, dx in shifts:
        pl.semaphore_signal(
            barrier, inc=1, device_id={"seq": seq_at(dy, dx)}, device_id_type=pl.DeviceIdType.MESH
        )
        pl.semaphore_signal(
            barrier,
            inc=1,
            device_id={"seq": seq_at(dy, dx), "kvh": other},
            device_id_type=pl.DeviceIdType.MESH,
        )
    for e in range(1, 8):
        pl.semaphore_signal(
            barrier, inc=1, device_id={"kvh": lax.rem(kvh + e, 8)}, device_id_type=pl.DeviceIdType.MESH
        )

    def where_true(cond):
        return jnp.where(cond, 1.0, 0.0).astype(BF16)

    wide_v[...] = jnp.full_like(wide_v, -1.0)
    col_v[...] = jnp.zeros_like(col_v)
    slot_v[...] = jnp.zeros_like(slot_v)
    with jax.named_scope("wait_ids"):
        l_ids.wait()
    wide_v[:, 0:64] = ids_v[...].astype(F32)
    ids = wide_v[...]
    first_id = (seq * 128).astype(F32)
    local = (ids >= first_id) & (ids < first_id + 128.0)
    block = ids - first_id
    hit = where_true(local)
    before = where_true(iota((16, 16), 1) < iota((16, 16), 0))
    counts = dot(jnp.ones((256, 16), BF16), hit)
    earlier = where_true(iota((128, 128), 0) < iota((128, 128), 1))
    rank = dot(counts[0:16].astype(BF16), earlier) + dot(before, hit)
    rank = jnp.where(local, rank, -1.0).astype(jnp.int32)
    high, low = rank >> 4, rank & 15
    digit = iota((16, 128), 0)
    token_at = iota((16, 128), 1).astype(F32)
    blocks, tokens, lows = [], [], []
    for s in range(16):
        same = high[s : s + 1, :] == digit
        blocks.append(jnp.where(same, block[s : s + 1, :], 0.0))
        tokens.append(jnp.where(same, token_at, 0.0))
        lows.append(jnp.where(low[s : s + 1, :] == digit, 1.0, 0.0))
    chosen = [jnp.concatenate(x, axis=1).astype(BF16) for x in (blocks, tokens, lows)]
    slots = dot_nt(chosen[2], jnp.concatenate(chosen[0:2], axis=0)).astype(jnp.int32)
    slot_v[:, 0:32] = slots & jnp.where(iota((16, 32), 1) < 16, 127, 63)
    to_smem = pltpu.make_async_copy(slot_v, slot_s, slot_sem)
    to_smem.start()
    cnt_v[...] = counts[0:8]
    counts = counts.astype(BF16)
    base = dot_nt(where_true(iota((64, 128), 1) < iota((64, 128), 0)), counts)
    count = dot_nt(where_true(iota((64, 128), 1) == iota((64, 128), 0)), counts)
    at = iota((64, 256), 1).astype(F32)
    tmap = jnp.where((at >= base) & (at < base + count), 1.0, 0.0)
    slot_token = jnp.sum(tmap * (iota((64, 256), 0) + 1).astype(F32), axis=0, keepdims=True)
    seg_v[...] = jnp.broadcast_to(slot_token, (8, 256))
    tmap_v[0] = tmap.astype(BF16)
    tmap_v[1] = where_true((at == base) & (count > 0.0))
    tmap_v[2] = where_true(count > 0.0)

    with jax.named_scope("wait_q"):
        wait_for(small_v, in_sem.at[2])
    wide = small_v[0].astype(F32)
    q3[...] = wide.reshape(64, 8, 128)
    q32[0:512, :] = wide
    for h in range(8):
        qh_v[h * 64 : h * 64 + 64, :] = q32[pl.ds(h, 64, stride=8), :].astype(BF16)
    rs_v[...] = dot_nt(qh_v[...], small_v[1])
    for h in range(8):
        s = rs_v[h * 64 : h * 64 + 64, :] * scale
        m = jnp.max(s, axis=1, keepdims=True)
        p = jnp.exp(s - m)
        rp_v[h * 64 : h * 64 + 64, :] = p.astype(BF16)
        col_v[0:64, h : h + 1] = m
        col_v[0:64, 8 + h : 9 + h] = jnp.sum(p, axis=1, keepdims=True)
    summed_v[...] = dot(rp_v[...], small_v[2])
    row_v[...] = col_v[...].T[0:16, :]

    lane = iota((8, 128), 1)
    empty = jnp.zeros((8, 128), F32)

    def beside(a, b):
        return jnp.concatenate([a, b], axis=1)

    def four(a, b, c, d):
        rows = [beside(a, empty), beside(empty, b), beside(c, empty), beside(empty, d)]
        return jnp.concatenate(rows, axis=0).astype(BF16)

    def apart(r):
        return r[0:8, 0:128], r[8:16, 0:128], r[16:24, 128:256], r[24:32, 128:256]

    with jax.named_scope("wait_smem"):
        l_cnt.wait()
        to_smem.wait()
    with jax.named_scope("wait_k"):
        l_k.wait()
    tops, totals = [empty, empty], [empty, empty]
    for j in range(0, CAP, 4):
        own = range(4)
        half = j // 128
        blk = [slot_s[j % 16 + i, j // 16] for i in own]
        query = [q3[slot_s[j % 16 + i, 16 + j // 16]] for i in own]
        tile = [k_v[blk[i]] for i in own]
        tile = jnp.concatenate([beside(tile[0], tile[1]), beside(tile[2], tile[3])], axis=0)
        found = apart(dot_nt(four(*query), tile))
        ps = []
        for i in own:
            here = lane == (j + i) % 128
            s = jnp.where(lane < cnt_s[blk[i]], found[i] * scale, FLOOR)
            m = jnp.max(s, axis=1, keepdims=True)
            p = jnp.exp(s - m)
            tops[half] = jnp.where(here, m, tops[half])
            totals[half] = jnp.where(here, jnp.sum(p, axis=1, keepdims=True), totals[half])
            ps.append(p)
        weight_v[j // 4] = four(*ps)
    with jax.named_scope("wait_v"):
        l_v.wait()
    for j in range(0, CAP, 4):
        tile = [v_v[slot_s[j % 16 + i, j // 16]] for i in own]
        tile = jnp.concatenate([beside(tile[0], tile[2]), beside(tile[1], tile[3])], axis=0)
        found = apart(dot(weight_v[j // 4], tile))
        for i in own:
            acc_v[pl.ds(j + i, 8, stride=STRIDE), :] = found[i]

    top, total = beside(*tops), beside(*totals)
    token = seg_v[...]
    most = top
    for back in (False, True):
        for k in (1, 2, 4, 8):
            by = 256 - k if back else k
            same = pltpu.roll(token, by, 1) == token
            most = jnp.maximum(most, jnp.where(same, pltpu.roll(most, by, 1), FLOOR))
    tmap_b, first_b = tmap_v[0], tmap_v[1]
    sum_m, sum_l = row_v[0:8, 0:64], row_v[8:16, 0:64]
    most = jnp.maximum(most, dot(sum_m.astype(BF16), tmap_b)).astype(BF16)
    shrink = jnp.exp(top - most.astype(F32))
    total = total * shrink
    total_hi = total.astype(BF16)
    total_lo = (total - total_hi.astype(F32)).astype(BF16)
    high = jnp.where(
        cnt_v[:, 0:64] > 0.0, dot_nt(most, first_b), sum_m.astype(BF16).astype(F32)
    )
    sums = dot_nt(total_hi, tmap_b) + dot_nt(total_lo, tmap_b) + sum_l * jnp.exp(sum_m - high)
    for y in range(4):
        zsend_v[y, :, 0:64] = high[2 * y : 2 * y + 2]
        zsend_v[y, :, 64:128] = sums[2 * y : 2 * y + 2]
    col_m = col_v[0:64, 0:8]
    high_col = jnp.where(
        tmap_v[2][:, 0:8].astype(F32) > 0.0, dot_nt(first_b, most), col_m.astype(BF16).astype(F32)
    )
    factor = jnp.exp(col_m - high_col)
    tmap_f = tmap_b[:, 0:CAP].astype(F32)
    lane8 = iota((64, 8), 1)
    for h in range(8):
        mine = (tmap_f * shrink[h : h + 1, 0:CAP]).astype(BF16)
        a = dot(mine, acc_v[h * STRIDE : h * STRIDE + CAP, :].astype(BF16))
        keep = jnp.sum(jnp.where(lane8 == h, factor, 0.0), axis=1, keepdims=True)
        a = (a + summed_v[h * 64 : h * 64 + 64, :] * keep).astype(BF16)
        for t in range(4):
            send_v[(h // 2) * 4 + t, h % 2] = a[t * 16 : t * 16 + 16]

    with jax.named_scope("barrier"):
        pl.semaphore_wait(barrier, 37)

    def remote(src, dst, send_sem, recv_sem, where):
        return pltpu.make_async_remote_copy(
            src_ref=src, dst_ref=dst, send_sem=send_sem, recv_sem=recv_sem,
            device_id=where, device_id_type=pl.DeviceIdType.MESH,
        )

    order = sorted(shifts, key=lambda d: -(min(d[0], 4 - d[0]) + min(d[1], 4 - d[1])))

    def give(dy, dx):
        d = dy * 4 + dx
        peer = seq_at(dy, dx)
        at = {"seq": peer, "kvh": keeper}
        remote(
            zsend_v.at[peer // 4], zrecv_v.at[core, d], rz_s, rz_r.at[core], at
        ).start()
        remote(send_v.at[peer], recv_v.at[core, d], rs_s, rs_r.at[core], at).start()

    for dy, dx in order:
        give(dy, dx)

    @pl.when(core == 0)
    def _():
        give(0, 0)

    def place(o):
        return att_v.at[pl.ds(2 * (o // 4), 2), pl.ds(pl.multiple_of(16 * (o % 4), 16), 16), :]

    def combined(group):
        heads = []
        for e in range(2):
            z = jnp.concatenate([zrecv_v[group, d, e : e + 1, :] for d in range(16)], axis=0)
            f = jnp.exp(z - jnp.max(z, axis=0, keepdims=True))
            f = jnp.where(iota((16, 128), 1) < 64, f, 0.0)
            whole = jnp.sum(f * pltpu.roll(z, 64, 1), axis=0, keepdims=True)
            g = jnp.where(iota((16, 128), 1) < 64, f / whole, 0.0)
            g_hi = g.astype(BF16)
            g_lo = (g - g_hi.astype(F32)).astype(BF16)
            share = dot_nt(pick, g_hi) + dot_nt(pick, g_lo)
            found = jnp.zeros((16, 128), F32)
            for d in range(16):
                part = jnp.where(iota((16, 16), 1) == d, share, 0.0)
                found = found + recv_v[group, d, e].astype(F32) * jnp.sum(
                    part, axis=1, keepdims=True
                )
            piece_v[group, e] = found.astype(BF16)

    pick = where_true(iota((16, 128), 1) == iota((16, 128), 0) + 16 * sx)

    @pl.when(core == 1)
    def _():
        with jax.named_scope("rs_recv0"):
            wait_for(zrecv_v.at[0], rz_r.at[0])
            wait_for(recv_v.at[0], rs_r.at[0])
        combined(0)
        for dy, dx in order + [(0, 0)]:
            at = {"seq": seq_at(dy, dx), "kvh": other}
            remote(piece_v.at[0], place(seq), ag_s.at[0], ag_r.at[sx], at).start()
        recv_v[1, 0] = send_v[seq]
        zrecv_v[1, 0] = zsend_v[sy]
        with jax.named_scope("rs_recv1"):
            wait_for(zrecv_v.at[1, pl.ds(1, 15)], rz_r.at[1])
            wait_for(recv_v.at[1, pl.ds(1, 15)], rs_r.at[1])
        combined(1)
        for dy, dx in order:
            at = {"seq": seq_at(dy, dx)}
            remote(piece_v.at[1], place(seq), ag_s.at[1], ag_r.at[sx], at).start()
        place(seq)[...] = piece_v[1]

    l_w.wait()

    for c in range(4):
        tokens = pl.ds(16 * c, 16)
        short = (core == 1) & (sx == c)
        with jax.named_scope(f"ag_recv{c}"):

            @pl.when(short)
            def _():
                wait_for(att_v.at[pl.ds(0, 6), tokens], ag_r.at[c])

            @pl.when(jnp.logical_not(short))
            def _():
                wait_for(att_v.at[:, tokens], ag_r.at[c])

        rows = jnp.concatenate([att_v[h, 16 * c : 16 * c + 16, :] for h in range(8)], axis=1)
        terms = dot(rows, w_v[...])
        for i in range(2):
            peer = 2 * c + i
            psend_v[peer] = terms[i * 8 : i * 8 + 8].astype(BF16)
            e = lax.rem(peer - kvh + 8, 8)

            @pl.when(kvh != peer)
            def _():
                remote(psend_v.at[peer], precv_v.at[e], pj_s, pj_r, {"kvh": peer}).start()

    @pl.when(core == 0)
    def _():
        wait_for(zrecv_v.at[0], rz_s)
        wait_for(recv_v.at[0], rs_s)

    @pl.when(core == 1)
    def _():
        wait_for(zrecv_v.at[1, pl.ds(1, 15)], rz_s)
        wait_for(recv_v.at[1, pl.ds(1, 15)], rs_s)
        wait_for(recv_v.at[0], ag_s.at[0])
        wait_for(recv_v.at[1, pl.ds(1, 15)], ag_s.at[1])

    result = psend_v[kvh].astype(F32)
    with jax.named_scope("pj_recv"):
        wait_for(precv_v.at[pl.ds(1, 7)], pj_r)
    for e in range(1, 8):
        result = result + precv_v[e].astype(F32)
    out_ref[...] = result.astype(BF16)
    with jax.named_scope("pj_send"):
        wait_for(psend_v.at[pl.ds(1, 7)], pj_s)


def on_device(queries, keys, values, rep_keys, rep_values, block_ids, block_counts, out_weight):
    vmem, smem, dma = pltpu.VMEM, pltpu.SMEM, pltpu.SemaphoreType.DMA
    any_spec = pl.BlockSpec(memory_space=pltpu.HBM)
    return pl.pallas_call(
        kernel,
        out_shape=jax.ShapeDtypeStruct((8, 512), BF16),
        in_specs=[any_spec] * 8,
        out_specs=pl.BlockSpec(memory_space=pltpu.VMEM),
        scratch_shapes=[
            vmem((3, 512, 128), BF16), vmem((128, 128, 128), BF16), vmem((128, 128, 128), BF16),
            vmem((16, 64), jnp.int32),
            vmem((1024, 512), BF16), smem((128,), jnp.int32), vmem((16, 128), jnp.int32),
            smem((16, 128), jnp.int32),
            vmem((16, 128), F32), vmem((64, 8, 128), F32), vmem((520, 128), F32),
            vmem((512, 128), BF16), vmem((512, 512), F32), vmem((512, 512), BF16), vmem((CAP // 4, 32, 256), BF16),
            vmem((9 * STRIDE, 128), F32), vmem((512, 128), F32), vmem((8, 256), F32),
            vmem((3, 64, 256), BF16), vmem((128, 128), F32), vmem((16, 128), F32),
            vmem((8, 128), F32),
            vmem((16, 2, 16, 128), BF16), vmem((2, 16, 2, 16, 128), BF16),
            vmem((4, 2, 128), F32), vmem((2, 16, 2, 128), F32), vmem((2, 2, 16, 128), BF16),
            vmem((8, 64, 128), BF16), vmem((8, 8, 512), BF16), vmem((8, 8, 512), BF16),
            dma((6,)), dma, dma, dma((2,)), dma, dma((2,)), dma((2,)), dma((4,)), dma, dma,
        ],
        compiler_params=pltpu.CompilerParams(collective_id=0, has_side_effects=True, vmem_limit_bytes=24 * 1024 * 1024),
        name="decode",
    )(*[pltpu.with_memory_space_constraint(x, pltpu.HBM) for x in (
        queries.reshape(-1, queries.shape[2]),
        keys.reshape(keys.shape[0], keys.shape[2], keys.shape[3]),
        values.reshape(values.shape[0], values.shape[2], values.shape[3]),
        rep_keys.reshape(-1, rep_keys.shape[3]),
        rep_values.reshape(-1, rep_values.shape[3]),
        jnp.transpose(block_ids, (1, 2, 0)).reshape(block_ids.shape[2], block_ids.shape[0]),
        block_counts,
        out_weight,
    )])


def solution(mesh):
    in_specs = (
        P(None, "kvh", None),
        P("seq", "kvh", None, None),
        P("seq", "kvh", None, None),
        P("seq", "kvh", None, None),
        P("seq", "kvh", None, None),
        P(None, "kvh", None),
        P("seq"),
        P("kvh", "seq"),
    )
    return jax.shard_map(
        on_device, mesh=mesh, in_specs=in_specs, out_specs=P("kvh", "seq"), check_vma=False
    )
```

```python
import functools
import math

import jax
import jax.numpy as jnp
from jax import lax
from jax.experimental import pallas as pl
from jax.experimental.pallas import tpu as pltpu
from jax.sharding import PartitionSpec as P

CAP = 192
STRIDE = 196
FLOOR = -1e30
F32 = jnp.float32
BF16 = jnp.bfloat16
NT = (((1,), (1,)), ((), ()))


def dot(a, b):
    return jnp.dot(a, b, preferred_element_type=F32)


def dot_nt(a, b):
    return lax.dot_general(a, b, NT, preferred_element_type=F32)


def iota(shape, dim):
    return lax.broadcasted_iota(jnp.int32, shape, dim)


def kernel(
    q_hbm, k_hbm, v_hbm, rk_hbm, rv_hbm, ids_hbm, cnt_hbm, w_hbm,
    out_ref,
    small_v, k_v, v_v, ids_v, w_v, cnt_s, slot_v, slot_s,
    wide_v, q3, q32, qh_v, rs_v, rp_v, weight_v, acc_v, summed_v, seg_v,
    tmap_v, col_v, row_v, cnt_v, send_v, recv_v, zsend_v, zrecv_v, piece_v, att_v, psend_v, precv_v,
    in_sem, slot_sem, rs_s, rs_r, rz_s, rz_r, ag_s, ag_r, pj_s, pj_r,
):
    seq = lax.axis_index("seq")
    kvh = lax.axis_index("kvh")
    sy, sx = seq // 4, seq % 4
    core = lax.rem(kvh, 2)
    other = kvh + 1 - 2 * core
    keeper = kvh + 1 - core
    scale = 1.0 / math.sqrt(128)

    def seq_at(dy, dx):
        return lax.rem(sy + dy + 4, 4) * 4 + lax.rem(sx + dx + 4, 4)

    shifts = [(dy, dx) for dy in range(4) for dx in range(4) if dy or dx]

    barrier = pltpu.get_barrier_semaphore()
    loads = [
        pltpu.make_async_copy(src, dst, in_sem.at[i])
        for src, dst, i in [
            (ids_hbm, ids_v, 0), (cnt_hbm, cnt_s, 1), (q_hbm, small_v.at[0], 2),
            (rk_hbm, small_v.at[1], 2), (rv_hbm, small_v.at[2], 2), (k_hbm, k_v, 3),
            (v_hbm, v_v, 4), (w_hbm, w_v, 5),
        ]
    ]
    for load in loads:
        load.start()
    l_ids, l_cnt, _, _, _, l_k, l_v, l_w = loads

    def wait_for(like, sem):
        pltpu.make_async_copy(like, like, sem).wait()

    for dy, dx in shifts:
        pl.semaphore_signal(
            barrier, inc=1, device_id={"seq": seq_at(dy, dx)}, device_id_type=pl.DeviceIdType.MESH
        )
        pl.semaphore_signal(
            barrier,
            inc=1,
            device_id={"seq": seq_at(dy, dx), "kvh": other},
            device_id_type=pl.DeviceIdType.MESH,
        )
    for e in range(1, 8):
        pl.semaphore_signal(
            barrier, inc=1, device_id={"kvh": lax.rem(kvh + e, 8)}, device_id_type=pl.DeviceIdType.MESH
        )

    def where_true(cond):
        return jnp.where(cond, 1.0, 0.0).astype(BF16)

    wide_v[...] = jnp.full_like(wide_v, -1.0)
    col_v[...] = jnp.zeros_like(col_v)
    slot_v[...] = jnp.zeros_like(slot_v)
    with jax.named_scope("wait_ids"):
        l_ids.wait()
    wide_v[:, 0:64] = ids_v[...].astype(F32)
    ids = wide_v[...]
    first_id = (seq * 128).astype(F32)
    local = (ids >= first_id) & (ids < first_id + 128.0)
    block = ids - first_id
    hit = where_true(local)
    before = where_true(iota((16, 16), 1) < iota((16, 16), 0))
    counts = dot(jnp.ones((256, 16), BF16), hit)
    earlier = where_true(iota((128, 128), 0) < iota((128, 128), 1))
    rank = dot(counts[0:16].astype(BF16), earlier) + dot(before, hit)
    rank = jnp.where(local, rank, -1.0).astype(jnp.int32)
    high, low = rank >> 4, rank & 15
    digit = iota((16, 128), 0)
    token_at = iota((16, 128), 1).astype(F32)
    blocks, tokens, lows = [], [], []
    for s in range(16):
        same = high[s : s + 1, :] == digit
        blocks.append(jnp.where(same, block[s : s + 1, :], 0.0))
        tokens.append(jnp.where(same, token_at, 0.0))
        lows.append(jnp.where(low[s : s + 1, :] == digit, 1.0, 0.0))
    chosen = [jnp.concatenate(x, axis=1).astype(BF16) for x in (blocks, tokens, lows)]
    slots = dot_nt(chosen[2], jnp.concatenate(chosen[0:2], axis=0)).astype(jnp.int32)
    slot_v[:, 0:32] = slots & jnp.where(iota((16, 32), 1) < 16, 127, 63)
    to_smem = pltpu.make_async_copy(slot_v, slot_s, slot_sem)
    to_smem.start()
    cnt_v[...] = counts[0:8]
    counts = counts.astype(BF16)
    base = dot_nt(where_true(iota((64, 128), 1) < iota((64, 128), 0)), counts)
    count = dot_nt(where_true(iota((64, 128), 1) == iota((64, 128), 0)), counts)
    at = iota((64, 256), 1).astype(F32)
    tmap = jnp.where((at >= base) & (at < base + count), 1.0, 0.0)
    slot_token = jnp.sum(tmap * (iota((64, 256), 0) + 1).astype(F32), axis=0, keepdims=True)
    seg_v[...] = jnp.broadcast_to(slot_token, (8, 256))
    tmap_v[0] = tmap.astype(BF16)
    tmap_v[1] = where_true((at == base) & (count > 0.0))
    tmap_v[2] = where_true(count > 0.0)

    with jax.named_scope("wait_q"):
        wait_for(small_v, in_sem.at[2])
    wide = small_v[0].astype(F32)
    q3[...] = wide.reshape(64, 8, 128)
    q32[0:512, :] = wide
    for h in range(8):
        qh_v[h * 64 : h * 64 + 64, :] = q32[pl.ds(h, 64, stride=8), :].astype(BF16)
    rs_v[...] = dot_nt(qh_v[...], small_v[1])
    for h in range(8):
        s = rs_v[h * 64 : h * 64 + 64, :] * scale
        m = jnp.max(s, axis=1, keepdims=True)
        p = jnp.exp(s - m)
        rp_v[h * 64 : h * 64 + 64, :] = p.astype(BF16)
        col_v[0:64, h : h + 1] = m
        col_v[0:64, 8 + h : 9 + h] = jnp.sum(p, axis=1, keepdims=True)
    summed_v[...] = dot(rp_v[...], small_v[2])
    row_v[...] = col_v[...].T[0:16, :]

    lane = iota((8, 128), 1)
    empty = jnp.zeros((8, 128), F32)

    def beside(a, b):
        return jnp.concatenate([a, b], axis=1)

    def four(a, b, c, d):
        rows = [beside(a, empty), beside(empty, b), beside(c, empty), beside(empty, d)]
        return jnp.concatenate(rows, axis=0).astype(BF16)

    def apart(r):
        return r[0:8, 0:128], r[8:16, 0:128], r[16:24, 128:256], r[24:32, 128:256]

    with jax.named_scope("wait_smem"):
        l_cnt.wait()
        to_smem.wait()
    with jax.named_scope("wait_k"):
        l_k.wait()
    tops, totals = [empty, empty], [empty, empty]
    for j in range(0, CAP, 4):
        own = range(4)
        half = j // 128
        blk = [slot_s[j % 16 + i, j // 16] for i in own]
        query = [q3[slot_s[j % 16 + i, 16 + j // 16]] for i in own]
        tile = [k_v[blk[i]] for i in own]
        tile = jnp.concatenate([beside(tile[0], tile[1]), beside(tile[2], tile[3])], axis=0)
        found = apart(dot_nt(four(*query), tile))
        ps = []
        for i in own:
            here = lane == (j + i) % 128
            s = jnp.where(lane < cnt_s[blk[i]], found[i] * scale, FLOOR)
            m = jnp.max(s, axis=1, keepdims=True)
            p = jnp.exp(s - m)
            tops[half] = jnp.where(here, m, tops[half])
            totals[half] = jnp.where(here, jnp.sum(p, axis=1, keepdims=True), totals[half])
            ps.append(p)
        weight_v[j // 4] = four(*ps)
    with jax.named_scope("wait_v"):
        l_v.wait()
    for j in range(0, CAP, 4):
        tile = [v_v[slot_s[j % 16 + i, j // 16]] for i in own]
        tile = jnp.concatenate([beside(tile[0], tile[2]), beside(tile[1], tile[3])], axis=0)
        found = apart(dot(weight_v[j // 4], tile))
        for i in own:
            acc_v[pl.ds(j + i, 8, stride=STRIDE), :] = found[i]

    top, total = beside(*tops), beside(*totals)
    token = seg_v[...]
    most = top
    for back in (False, True):
        for k in (1, 2, 4, 8):
            by = 256 - k if back else k
            same = pltpu.roll(token, by, 1) == token
            most = jnp.maximum(most, jnp.where(same, pltpu.roll(most, by, 1), FLOOR))
    tmap_b, first_b = tmap_v[0], tmap_v[1]
    sum_m, sum_l = row_v[0:8, 0:64], row_v[8:16, 0:64]
    most = jnp.maximum(most, dot(sum_m.astype(BF16), tmap_b)).astype(BF16)
    shrink = jnp.exp(top - most.astype(F32))
    total = total * shrink
    total_hi = total.astype(BF16)
    total_lo = (total - total_hi.astype(F32)).astype(BF16)
    high = jnp.where(
        cnt_v[:, 0:64] > 0.0, dot_nt(most, first_b), sum_m.astype(BF16).astype(F32)
    )
    sums = dot_nt(total_hi, tmap_b) + dot_nt(total_lo, tmap_b) + sum_l * jnp.exp(sum_m - high)
    for y in range(4):
        zsend_v[y, :, 0:64] = high[2 * y : 2 * y + 2]
        zsend_v[y, :, 64:128] = sums[2 * y : 2 * y + 2]
    col_m = col_v[0:64, 0:8]
    high_col = jnp.where(
        tmap_v[2][:, 0:8].astype(F32) > 0.0, dot_nt(first_b, most), col_m.astype(BF16).astype(F32)
    )
    factor = jnp.exp(col_m - high_col)
    tmap_f = tmap_b[:, 0:CAP].astype(F32)
    lane8 = iota((64, 8), 1)
    for h in range(8):
        mine = (tmap_f * shrink[h : h + 1, 0:CAP]).astype(BF16)
        a = dot(mine, acc_v[h * STRIDE : h * STRIDE + CAP, :].astype(BF16))
        keep = jnp.sum(jnp.where(lane8 == h, factor, 0.0), axis=1, keepdims=True)
        a = (a + summed_v[h * 64 : h * 64 + 64, :] * keep).astype(BF16)
        for t in range(4):
            send_v[(h // 2) * 4 + t, h % 2] = a[t * 16 : t * 16 + 16]

    with jax.named_scope("barrier"):
        pl.semaphore_wait(barrier, 37)

    def remote(src, dst, send_sem, recv_sem, where):
        return pltpu.make_async_remote_copy(
            src_ref=src, dst_ref=dst, send_sem=send_sem, recv_sem=recv_sem,
            device_id=where, device_id_type=pl.DeviceIdType.MESH,
        )

    order = sorted(shifts, key=lambda d: -(min(d[0], 4 - d[0]) + min(d[1], 4 - d[1])))

    def give(dy, dx):
        d = dy * 4 + dx
        peer = seq_at(dy, dx)
        at = {"seq": peer, "kvh": keeper}
        remote(
            zsend_v.at[peer // 4], zrecv_v.at[core, d], rz_s, rz_r.at[core], at
        ).start()
        remote(send_v.at[peer], recv_v.at[core, d], rs_s, rs_r.at[core], at).start()

    for c in range(4):
        for dy in (2, 1, 3, 0):

            @pl.when((core == 0) | (sx != c) | (dy != 0))
            def _():
                give(dy, lax.rem(c - sx + 4, 4))

    def place(o):
        return att_v.at[pl.ds(2 * (o // 4), 2), pl.ds(pl.multiple_of(16 * (o % 4), 16), 16), :]

    def combined(group):
        heads = []
        for e in range(2):
            z = zrecv_v[group, :, e, :]
            f = jnp.exp(z - jnp.max(z, axis=0, keepdims=True))
            f = jnp.where(iota((16, 128), 1) < 64, f, 0.0)
            whole = jnp.sum(f * pltpu.roll(z, 64, 1), axis=0, keepdims=True)
            g = jnp.where(iota((16, 128), 1) < 64, f / whole, 0.0)
            g_hi = g.astype(BF16)
            g_lo = (g - g_hi.astype(F32)).astype(BF16)
            share = dot_nt(pick, g_hi) + dot_nt(pick, g_lo)
            found = jnp.zeros((16, 128), F32)
            for d in range(16):
                part = jnp.where(iota((16, 16), 1) == d, share, 0.0)
                found = found + recv_v[group, d, e].astype(F32) * jnp.sum(
                    part, axis=1, keepdims=True
                )
            piece_v[group, e] = found.astype(BF16)

    pick = where_true(iota((16, 128), 1) == iota((16, 128), 0) + 16 * sx)

    @pl.when(core == 1)
    def _():
        recv_v[1, 0] = send_v[seq]
        zrecv_v[1, 0] = zsend_v[sy]
        with jax.named_scope("rs_recv1"):
            wait_for(zrecv_v.at[1, pl.ds(1, 15)], rz_r.at[1])
            wait_for(recv_v.at[1, pl.ds(1, 15)], rs_r.at[1])
        combined(1)
        for dy, dx in order:
            at = {"seq": seq_at(dy, dx)}
            remote(piece_v.at[1], place(seq), ag_s.at[1], ag_r.at[sx], at).start()
        place(seq)[...] = piece_v[1]
        with jax.named_scope("rs_recv0"):
            wait_for(zrecv_v.at[0], rz_r.at[0])
            wait_for(recv_v.at[0], rs_r.at[0])
        combined(0)
        for dy, dx in order + [(0, 0)]:
            at = {"seq": seq_at(dy, dx), "kvh": other}
            remote(piece_v.at[0], place(seq), ag_s.at[0], ag_r.at[sx], at).start()

    l_w.wait()

    for c in range(4):
        tokens = pl.ds(16 * c, 16)
        short = (core == 1) & (sx == c)
        with jax.named_scope(f"ag_recv{c}"):

            @pl.when(short)
            def _():
                wait_for(att_v.at[pl.ds(0, 6), tokens], ag_r.at[c])

            @pl.when(jnp.logical_not(short))
            def _():
                wait_for(att_v.at[:, tokens], ag_r.at[c])

        rows = jnp.concatenate([att_v[h, 16 * c : 16 * c + 16, :] for h in range(8)], axis=1)
        terms = dot(rows, w_v[...])
        for i in range(2):
            peer = 2 * c + i
            psend_v[peer] = terms[i * 8 : i * 8 + 8].astype(BF16)
            e = lax.rem(peer - kvh + 8, 8)

            @pl.when(kvh != peer)
            def _():
                remote(psend_v.at[peer], precv_v.at[e], pj_s, pj_r, {"kvh": peer}).start()

    @pl.when(core == 0)
    def _():
        wait_for(zrecv_v.at[0], rz_s)
        wait_for(recv_v.at[0], rs_s)

    @pl.when(core == 1)
    def _():
        wait_for(zrecv_v.at[1, pl.ds(1, 15)], rz_s)
        wait_for(recv_v.at[1, pl.ds(1, 15)], rs_s)
        wait_for(recv_v.at[0], ag_s.at[0])
        wait_for(recv_v.at[1, pl.ds(1, 15)], ag_s.at[1])

    result = psend_v[kvh].astype(F32)
    with jax.named_scope("pj_recv"):
        wait_for(precv_v.at[pl.ds(1, 7)], pj_r)
    for e in range(1, 8):
        result = result + precv_v[e].astype(F32)
    out_ref[...] = result.astype(BF16)
    with jax.named_scope("pj_send"):
        wait_for(psend_v.at[pl.ds(1, 7)], pj_s)


def on_device(queries, keys, values, rep_keys, rep_values, block_ids, block_counts, out_weight):
    vmem, smem, dma = pltpu.VMEM, pltpu.SMEM, pltpu.SemaphoreType.DMA
    any_spec = pl.BlockSpec(memory_space=pltpu.HBM)
    return pl.pallas_call(
        kernel,
        out_shape=jax.ShapeDtypeStruct((8, 512), BF16),
        in_specs=[any_spec] * 8,
        out_specs=pl.BlockSpec(memory_space=pltpu.VMEM),
        scratch_shapes=[
            vmem((3, 512, 128), BF16), vmem((128, 128, 128), BF16), vmem((128, 128, 128), BF16),
            vmem((16, 64), jnp.int32),
            vmem((1024, 512), BF16), smem((128,), jnp.int32), vmem((16, 128), jnp.int32),
            smem((16, 128), jnp.int32),
            vmem((16, 128), F32), vmem((64, 8, 128), F32), vmem((520, 128), F32),
            vmem((512, 128), BF16), vmem((512, 512), F32), vmem((512, 512), BF16), vmem((CAP // 4, 32, 256), BF16),
            vmem((9 * STRIDE, 128), F32), vmem((512, 128), F32), vmem((8, 256), F32),
            vmem((3, 64, 256), BF16), vmem((128, 128), F32), vmem((16, 128), F32),
            vmem((8, 128), F32),
            vmem((16, 2, 16, 128), BF16), vmem((2, 16, 2, 16, 128), BF16),
            vmem((4, 2, 128), F32), vmem((2, 16, 2, 128), F32), vmem((2, 2, 16, 128), BF16),
            vmem((8, 64, 128), BF16), vmem((8, 8, 512), BF16), vmem((8, 8, 512), BF16),
            dma((6,)), dma, dma, dma((2,)), dma, dma((2,)), dma((2,)), dma((4,)), dma, dma,
        ],
        compiler_params=pltpu.CompilerParams(collective_id=0, has_side_effects=True, vmem_limit_bytes=24 * 1024 * 1024),
        name="decode",
    )(*[pltpu.with_memory_space_constraint(x, pltpu.HBM) for x in (
        queries.reshape(-1, queries.shape[2]),
        keys.reshape(keys.shape[0], keys.shape[2], keys.shape[3]),
        values.reshape(values.shape[0], values.shape[2], values.shape[3]),
        rep_keys.reshape(-1, rep_keys.shape[3]),
        rep_values.reshape(-1, rep_values.shape[3]),
        jnp.transpose(block_ids, (1, 2, 0)).reshape(block_ids.shape[2], block_ids.shape[0]),
        block_counts,
        out_weight,
    )])


def solution(mesh):
    in_specs = (
        P(None, "kvh", None),
        P("seq", "kvh", None, None),
        P("seq", "kvh", None, None),
        P("seq", "kvh", None, None),
        P("seq", "kvh", None, None),
        P(None, "kvh", None),
        P("seq"),
        P("kvh", "seq"),
    )
    return jax.shard_map(
        on_device, mesh=mesh, in_specs=in_specs, out_specs=P("kvh", "seq"), check_vma=False
    )
```

```python
import functools
import math

import jax
import jax.numpy as jnp
from jax import lax
from jax.experimental import pallas as pl
from jax.experimental.pallas import tpu as pltpu
from jax.sharding import PartitionSpec as P

CAP = 192
STRIDE = 196
FLOOR = -1e30
F32 = jnp.float32
BF16 = jnp.bfloat16
NT = (((1,), (1,)), ((), ()))


def dot(a, b):
    return jnp.dot(a, b, preferred_element_type=F32)


def dot_nt(a, b):
    return lax.dot_general(a, b, NT, preferred_element_type=F32)


def iota(shape, dim):
    return lax.broadcasted_iota(jnp.int32, shape, dim)


def kernel(
    q_hbm, k_hbm, v_hbm, rk_hbm, rv_hbm, ids_hbm, cnt_hbm, w_hbm,
    out_ref,
    small_v, k_v, v_v, ids_v, w_v, cnt_s, slot_v, slot_s,
    wide_v, q3, q32, qh_v, rs_v, rp_v, weight_v, acc_v, summed_v, seg_v,
    tmap_v, col_v, row_v, cnt_v, send_v, recv_v, zsend_v, zrecv_v, piece_v, att_v, psend_v, precv_v,
    in_sem, slot_sem, rs_s, rs_r, rz_s, rz_r, ag_s, ag_r, pj_s, pj_r,
):
    seq = lax.axis_index("seq")
    kvh = lax.axis_index("kvh")
    sy, sx = seq // 4, seq % 4
    core = lax.rem(kvh, 2)
    other = kvh + 1 - 2 * core
    keeper = kvh + 1 - core
    scale = 1.0 / math.sqrt(128)

    def seq_at(dy, dx):
        return lax.rem(sy + dy + 4, 4) * 4 + lax.rem(sx + dx + 4, 4)

    shifts = [(dy, dx) for dy in range(4) for dx in range(4) if dy or dx]

    barrier = pltpu.get_barrier_semaphore()
    loads = [
        pltpu.make_async_copy(src, dst, in_sem.at[i])
        for src, dst, i in [
            (ids_hbm, ids_v, 0), (cnt_hbm, cnt_s, 1), (q_hbm, small_v.at[0], 2),
            (rk_hbm, small_v.at[1], 2), (rv_hbm, small_v.at[2], 2), (k_hbm, k_v, 3),
            (v_hbm, v_v, 4), (w_hbm, w_v, 5),
        ]
    ]
    for load in loads:
        load.start()
    l_ids, l_cnt, _, _, _, l_k, l_v, l_w = loads

    def wait_for(like, sem):
        pltpu.make_async_copy(like, like, sem).wait()

    for dy, dx in shifts:
        pl.semaphore_signal(
            barrier, inc=1, device_id={"seq": seq_at(dy, dx)}, device_id_type=pl.DeviceIdType.MESH
        )
        pl.semaphore_signal(
            barrier,
            inc=1,
            device_id={"seq": seq_at(dy, dx), "kvh": other},
            device_id_type=pl.DeviceIdType.MESH,
        )
    for e in range(1, 8):
        pl.semaphore_signal(
            barrier, inc=1, device_id={"kvh": lax.rem(kvh + e, 8)}, device_id_type=pl.DeviceIdType.MESH
        )

    def where_true(cond):
        return jnp.where(cond, 1.0, 0.0).astype(BF16)

    wide_v[...] = jnp.full_like(wide_v, -1.0)
    col_v[...] = jnp.zeros_like(col_v)
    slot_v[...] = jnp.zeros_like(slot_v)
    with jax.named_scope("wait_ids"):
        l_ids.wait()
    wide_v[:, 0:64] = ids_v[...].astype(F32)
    ids = wide_v[...]
    first_id = (seq * 128).astype(F32)
    local = (ids >= first_id) & (ids < first_id + 128.0)
    block = ids - first_id
    hit = where_true(local)
    before = where_true(iota((16, 16), 1) < iota((16, 16), 0))
    counts = dot(jnp.ones((256, 16), BF16), hit)
    earlier = where_true(iota((128, 128), 0) < iota((128, 128), 1))
    rank = dot(counts[0:16].astype(BF16), earlier) + dot(before, hit)
    rank = jnp.where(local, rank, -1.0).astype(jnp.int32)
    high, low = rank >> 4, rank & 15
    digit = iota((16, 128), 0)
    token_at = iota((16, 128), 1).astype(F32)
    blocks, tokens, lows = [], [], []
    for s in range(16):
        same = high[s : s + 1, :] == digit
        blocks.append(jnp.where(same, block[s : s + 1, :], 0.0))
        tokens.append(jnp.where(same, token_at, 0.0))
        lows.append(jnp.where(low[s : s + 1, :] == digit, 1.0, 0.0))
    chosen = [jnp.concatenate(x, axis=1).astype(BF16) for x in (blocks, tokens, lows)]
    slots = dot_nt(chosen[2], jnp.concatenate(chosen[0:2], axis=0)).astype(jnp.int32)
    slot_v[:, 0:32] = slots & jnp.where(iota((16, 32), 1) < 16, 127, 63)
    to_smem = pltpu.make_async_copy(slot_v, slot_s, slot_sem)
    to_smem.start()
    cnt_v[...] = counts[0:8]
    counts = counts.astype(BF16)
    base = dot_nt(where_true(iota((64, 128), 1) < iota((64, 128), 0)), counts)
    count = dot_nt(where_true(iota((64, 128), 1) == iota((64, 128), 0)), counts)
    at = iota((64, 256), 1).astype(F32)
    tmap = jnp.where((at >= base) & (at < base + count), 1.0, 0.0)
    slot_token = jnp.sum(tmap * (iota((64, 256), 0) + 1).astype(F32), axis=0, keepdims=True)
    seg_v[...] = jnp.broadcast_to(slot_token, (8, 256))
    tmap_v[0] = tmap.astype(BF16)
    tmap_v[1] = where_true((at == base) & (count > 0.0))
    tmap_v[2] = where_true(count > 0.0)

    with jax.named_scope("wait_q"):
        wait_for(small_v, in_sem.at[2])
    wide = small_v[0].astype(F32)
    q3[...] = wide.reshape(64, 8, 128)
    q32[0:512, :] = wide
    for h in range(8):
        qh_v[h * 64 : h * 64 + 64, :] = q32[pl.ds(h, 64, stride=8), :].astype(BF16)
    rs_v[...] = dot_nt(qh_v[...], small_v[1])
    for h in range(8):
        s = rs_v[h * 64 : h * 64 + 64, :] * scale
        m = jnp.max(s, axis=1, keepdims=True)
        p = jnp.exp(s - m)
        rp_v[h * 64 : h * 64 + 64, :] = p.astype(BF16)
        col_v[0:64, h : h + 1] = m
        col_v[0:64, 8 + h : 9 + h] = jnp.sum(p, axis=1, keepdims=True)
    summed_v[...] = dot(rp_v[...], small_v[2])
    row_v[...] = col_v[...].T[0:16, :]

    lane = iota((8, 128), 1)
    empty = jnp.zeros((8, 128), F32)

    def beside(a, b):
        return jnp.concatenate([a, b], axis=1)

    def four(a, b, c, d):
        rows = [beside(a, empty), beside(empty, b), beside(c, empty), beside(empty, d)]
        return jnp.concatenate(rows, axis=0).astype(BF16)

    def apart(r):
        return r[0:8, 0:128], r[8:16, 0:128], r[16:24, 128:256], r[24:32, 128:256]

    with jax.named_scope("wait_smem"):
        l_cnt.wait()
        to_smem.wait()
    with jax.named_scope("wait_k"):
        l_k.wait()
    tops, totals = [empty, empty], [empty, empty]
    for j in range(0, CAP, 4):
        own = range(4)
        half = j // 128
        blk = [slot_s[j % 16 + i, j // 16] for i in own]
        query = [q3[slot_s[j % 16 + i, 16 + j // 16]] for i in own]
        tile = [k_v[blk[i]] for i in own]
        tile = jnp.concatenate([beside(tile[0], tile[1]), beside(tile[2], tile[3])], axis=0)
        found = apart(dot_nt(four(*query), tile))
        ps = []
        for i in own:
            here = lane == (j + i) % 128
            s = jnp.where(lane < cnt_s[blk[i]], found[i] * scale, FLOOR)
            m = jnp.max(s, axis=1, keepdims=True)
            p = jnp.exp(s - m)
            tops[half] = jnp.where(here, m, tops[half])
            totals[half] = jnp.where(here, jnp.sum(p, axis=1, keepdims=True), totals[half])
            ps.append(p)
        weight_v[j // 4] = four(*ps)
    with jax.named_scope("wait_v"):
        l_v.wait()
    for j in range(0, CAP, 4):
        tile = [v_v[slot_s[j % 16 + i, j // 16]] for i in own]
        tile = jnp.concatenate([beside(tile[0], tile[2]), beside(tile[1], tile[3])], axis=0)
        found = apart(dot(weight_v[j // 4], tile))
        for i in own:
            acc_v[pl.ds(j + i, 8, stride=STRIDE), :] = found[i]

    top, total = beside(*tops), beside(*totals)
    token = seg_v[...]
    most = top
    for back in (False, True):
        for k in (1, 2, 4, 8):
            by = 256 - k if back else k
            same = pltpu.roll(token, by, 1) == token
            most = jnp.maximum(most, jnp.where(same, pltpu.roll(most, by, 1), FLOOR))
    tmap_b, first_b = tmap_v[0], tmap_v[1]
    sum_m, sum_l = row_v[0:8, 0:64], row_v[8:16, 0:64]
    most = jnp.maximum(most, dot(sum_m.astype(BF16), tmap_b)).astype(BF16)
    shrink = jnp.exp(top - most.astype(F32))
    total = total * shrink
    total_hi = total.astype(BF16)
    total_lo = (total - total_hi.astype(F32)).astype(BF16)
    high = jnp.where(
        cnt_v[:, 0:64] > 0.0, dot_nt(most, first_b), sum_m.astype(BF16).astype(F32)
    )
    sums = dot_nt(total_hi, tmap_b) + dot_nt(total_lo, tmap_b) + sum_l * jnp.exp(sum_m - high)
    for y in range(4):
        zsend_v[y, :, 0:64] = high[2 * y : 2 * y + 2]
        zsend_v[y, :, 64:128] = sums[2 * y : 2 * y + 2]
    with jax.named_scope("barrier"):
        pl.semaphore_wait(barrier, 37)

    def remote(src, dst, send_sem, recv_sem, where):
        return pltpu.make_async_remote_copy(
            src_ref=src, dst_ref=dst, send_sem=send_sem, recv_sem=recv_sem,
            device_id=where, device_id_type=pl.DeviceIdType.MESH,
        )

    order = sorted(shifts, key=lambda d: -(min(d[0], 4 - d[0]) + min(d[1], 4 - d[1])))

    def tell(dy, dx):
        peer = seq_at(dy, dx)
        at = {"seq": peer, "kvh": keeper}
        source = zsend_v.at[peer // 4]
        remote(source, zrecv_v.at[core, dy * 4 + dx], rz_s, rz_r.at[core], at).start()

    for dy, dx in shifts:
        tell(dy, dx)

    @pl.when(core == 0)
    def _():
        tell(0, 0)

    col_m = col_v[0:64, 0:8]
    high_col = jnp.where(
        tmap_v[2][:, 0:8].astype(F32) > 0.0, dot_nt(first_b, most), col_m.astype(BF16).astype(F32)
    )
    factor = jnp.exp(col_m - high_col)
    tmap_f = tmap_b[:, 0:CAP].astype(F32)
    lane8 = iota((64, 8), 1)
    for h in range(8):
        mine = (tmap_f * shrink[h : h + 1, 0:CAP]).astype(BF16)
        a = dot(mine, acc_v[h * STRIDE : h * STRIDE + CAP, :].astype(BF16))
        keep = jnp.sum(jnp.where(lane8 == h, factor, 0.0), axis=1, keepdims=True)
        a = (a + summed_v[h * 64 : h * 64 + 64, :] * keep).astype(BF16)
        for t in range(4):
            send_v[(h // 2) * 4 + t, h % 2] = a[t * 16 : t * 16 + 16]

    def give(dy, dx):
        d = dy * 4 + dx
        peer = seq_at(dy, dx)
        at = {"seq": peer, "kvh": keeper}
        remote(send_v.at[peer], recv_v.at[core, d], rs_s, rs_r.at[core], at).start()

    for c in range(4):
        for dy in (2, 1, 3, 0):

            @pl.when((core == 0) | (sx != c) | (dy != 0))
            def _():
                give(dy, lax.rem(c - sx + 4, 4))

    def place(o):
        return att_v.at[pl.ds(2 * (o // 4), 2), pl.ds(pl.multiple_of(16 * (o % 4), 16), 16), :]

    def combined(group):
        heads = []
        for e in range(2):
            z = zrecv_v[group, :, e, :]
            f = jnp.exp(z - jnp.max(z, axis=0, keepdims=True))
            f = jnp.where(iota((16, 128), 1) < 64, f, 0.0)
            whole = jnp.sum(f * pltpu.roll(z, 64, 1), axis=0, keepdims=True)
            g = jnp.where(iota((16, 128), 1) < 64, f / whole, 0.0)
            g_hi = g.astype(BF16)
            g_lo = (g - g_hi.astype(F32)).astype(BF16)
            share = dot_nt(pick, g_hi) + dot_nt(pick, g_lo)
            found = jnp.zeros((16, 128), F32)
            for d in range(16):
                part = jnp.where(iota((16, 16), 1) == d, share, 0.0)
                found = found + recv_v[group, d, e].astype(F32) * jnp.sum(
                    part, axis=1, keepdims=True
                )
            piece_v[group, e] = found.astype(BF16)

    pick = where_true(iota((16, 128), 1) == iota((16, 128), 0) + 16 * sx)

    @pl.when(core == 1)
    def _():
        recv_v[1, 0] = send_v[seq]
        zrecv_v[1, 0] = zsend_v[sy]
        with jax.named_scope("rs_recv1"):
            wait_for(zrecv_v.at[1, pl.ds(1, 15)], rz_r.at[1])
            wait_for(recv_v.at[1, pl.ds(1, 15)], rs_r.at[1])
        combined(1)
        for dy, dx in order:
            at = {"seq": seq_at(dy, dx)}
            remote(piece_v.at[1], place(seq), ag_s.at[1], ag_r.at[sx], at).start()
        place(seq)[...] = piece_v[1]
        with jax.named_scope("rs_recv0"):
            wait_for(zrecv_v.at[0], rz_r.at[0])
            wait_for(recv_v.at[0], rs_r.at[0])
        combined(0)
        for dy, dx in order + [(0, 0)]:
            at = {"seq": seq_at(dy, dx), "kvh": other}
            remote(piece_v.at[0], place(seq), ag_s.at[0], ag_r.at[sx], at).start()

    l_w.wait()

    for c in range(4):
        tokens = pl.ds(16 * c, 16)
        short = (core == 1) & (sx == c)
        with jax.named_scope(f"ag_recv{c}"):

            @pl.when(short)
            def _():
                wait_for(att_v.at[pl.ds(0, 6), tokens], ag_r.at[c])

            @pl.when(jnp.logical_not(short))
            def _():
                wait_for(att_v.at[:, tokens], ag_r.at[c])

        rows = jnp.concatenate([att_v[h, 16 * c : 16 * c + 16, :] for h in range(8)], axis=1)
        terms = dot(rows, w_v[...])
        for i in range(2):
            peer = 2 * c + i
            psend_v[peer] = terms[i * 8 : i * 8 + 8].astype(BF16)
            e = lax.rem(peer - kvh + 8, 8)

            @pl.when(kvh != peer)
            def _():
                remote(psend_v.at[peer], precv_v.at[e], pj_s, pj_r, {"kvh": peer}).start()

    @pl.when(core == 0)
    def _():
        wait_for(zrecv_v.at[0], rz_s)
        wait_for(recv_v.at[0], rs_s)

    @pl.when(core == 1)
    def _():
        wait_for(zrecv_v.at[1, pl.ds(1, 15)], rz_s)
        wait_for(recv_v.at[1, pl.ds(1, 15)], rs_s)
        wait_for(recv_v.at[0], ag_s.at[0])
        wait_for(recv_v.at[1, pl.ds(1, 15)], ag_s.at[1])

    result = psend_v[kvh].astype(F32)
    with jax.named_scope("pj_recv"):
        wait_for(precv_v.at[pl.ds(1, 7)], pj_r)
    for e in range(1, 8):
        result = result + precv_v[e].astype(F32)
    out_ref[...] = result.astype(BF16)
    with jax.named_scope("pj_send"):
        wait_for(psend_v.at[pl.ds(1, 7)], pj_s)


def on_device(queries, keys, values, rep_keys, rep_values, block_ids, block_counts, out_weight):
    vmem, smem, dma = pltpu.VMEM, pltpu.SMEM, pltpu.SemaphoreType.DMA
    any_spec = pl.BlockSpec(memory_space=pltpu.HBM)
    return pl.pallas_call(
        kernel,
        out_shape=jax.ShapeDtypeStruct((8, 512), BF16),
        in_specs=[any_spec] * 8,
        out_specs=pl.BlockSpec(memory_space=pltpu.VMEM),
        scratch_shapes=[
            vmem((3, 512, 128), BF16), vmem((128, 128, 128), BF16), vmem((128, 128, 128), BF16),
            vmem((16, 64), jnp.int32),
            vmem((1024, 512), BF16), smem((128,), jnp.int32), vmem((16, 128), jnp.int32),
            smem((16, 128), jnp.int32),
            vmem((16, 128), F32), vmem((64, 8, 128), F32), vmem((520, 128), F32),
            vmem((512, 128), BF16), vmem((512, 512), F32), vmem((512, 512), BF16), vmem((CAP // 4, 32, 256), BF16),
            vmem((9 * STRIDE, 128), F32), vmem((512, 128), F32), vmem((8, 256), F32),
            vmem((3, 64, 256), BF16), vmem((128, 128), F32), vmem((16, 128), F32),
            vmem((8, 128), F32),
            vmem((16, 2, 16, 128), BF16), vmem((2, 16, 2, 16, 128), BF16),
            vmem((4, 2, 128), F32), vmem((2, 16, 2, 128), F32), vmem((2, 2, 16, 128), BF16),
            vmem((8, 64, 128), BF16), vmem((8, 8, 512), BF16), vmem((8, 8, 512), BF16),
            dma((6,)), dma, dma, dma((2,)), dma, dma((2,)), dma((2,)), dma((4,)), dma, dma,
        ],
        compiler_params=pltpu.CompilerParams(collective_id=0, has_side_effects=True, vmem_limit_bytes=24 * 1024 * 1024),
        name="decode",
    )(*[pltpu.with_memory_space_constraint(x, pltpu.HBM) for x in (
        queries.reshape(-1, queries.shape[2]),
        keys.reshape(keys.shape[0], keys.shape[2], keys.shape[3]),
        values.reshape(values.shape[0], values.shape[2], values.shape[3]),
        rep_keys.reshape(-1, rep_keys.shape[3]),
        rep_values.reshape(-1, rep_values.shape[3]),
        jnp.transpose(block_ids, (1, 2, 0)).reshape(block_ids.shape[2], block_ids.shape[0]),
        block_counts,
        out_weight,
    )])


def solution(mesh):
    in_specs = (
        P(None, "kvh", None),
        P("seq", "kvh", None, None),
        P("seq", "kvh", None, None),
        P("seq", "kvh", None, None),
        P("seq", "kvh", None, None),
        P(None, "kvh", None),
        P("seq"),
        P("kvh", "seq"),
    )
    return jax.shard_map(
        on_device, mesh=mesh, in_specs=in_specs, out_specs=P("kvh", "seq"), check_vma=False
    )
```

```python
import functools
import math

import jax
import jax.numpy as jnp
from jax import lax
from jax.experimental import pallas as pl
from jax.experimental.pallas import tpu as pltpu
from jax.sharding import PartitionSpec as P

CAP = 192
STRIDE = 196
FLOOR = -1e30
F32 = jnp.float32
BF16 = jnp.bfloat16
NT = (((1,), (1,)), ((), ()))


def dot(a, b):
    return jnp.dot(a, b, preferred_element_type=F32)


def dot_nt(a, b):
    return lax.dot_general(a, b, NT, preferred_element_type=F32)


def iota(shape, dim):
    return lax.broadcasted_iota(jnp.int32, shape, dim)


def kernel(
    q_hbm, k_hbm, v_hbm, rk_hbm, rv_hbm, ids_hbm, cnt_hbm, w_hbm,
    out_ref,
    small_v, k_v, v_v, ids_v, w_v, cnt_s, slot_v, slot_s,
    wide_v, q3, q32, qh_v, rs_v, rp_v, weight_v, acc_v, summed_v, seg_v,
    tmap_v, col_v, row_v, cnt_v, send_v, recv_v, zsend_v, zrecv_v, piece_v, att_v, psend_v, precv_v,
    in_sem, slot_sem, rs_s, rs_r, rz_s, rz_r, ag_s, ag_r, pj_s, pj_r, w_s, w_r,
):
    seq = lax.axis_index("seq")
    kvh = lax.axis_index("kvh")
    sy, sx = seq // 4, seq % 4
    core = lax.rem(kvh, 2)
    other = kvh + 1 - 2 * core
    keeper = kvh + 1 - core
    scale = 1.0 / math.sqrt(128)

    def seq_at(dy, dx):
        return lax.rem(sy + dy + 4, 4) * 4 + lax.rem(sx + dx + 4, 4)

    shifts = [(dy, dx) for dy in range(4) for dx in range(4) if dy or dx]

    barrier = pltpu.get_barrier_semaphore()
    loads = [
        pltpu.make_async_copy(src, dst, in_sem.at[i])
        for src, dst, i in [
            (ids_hbm, ids_v, 0), (cnt_hbm, cnt_s, 1), (q_hbm, small_v.at[0], 2),
            (rk_hbm, small_v.at[1], 2), (rv_hbm, small_v.at[2], 2), (k_hbm, k_v, 3),
            (v_hbm, v_v, 4), (w_hbm, w_v.at[1], 5),
        ]
    ]
    for load in loads:
        load.start()
    l_ids, l_cnt, _, _, _, l_k, l_v, l_w = loads

    def wait_for(like, sem):
        pltpu.make_async_copy(like, like, sem).wait()

    for dy, dx in shifts:
        pl.semaphore_signal(
            barrier, inc=1, device_id={"seq": seq_at(dy, dx)}, device_id_type=pl.DeviceIdType.MESH
        )
        pl.semaphore_signal(
            barrier,
            inc=1,
            device_id={"seq": seq_at(dy, dx), "kvh": other},
            device_id_type=pl.DeviceIdType.MESH,
        )
    for e in range(1, 8):
        pl.semaphore_signal(
            barrier, inc=1, device_id={"kvh": lax.rem(kvh + e, 8)}, device_id_type=pl.DeviceIdType.MESH
        )

    def where_true(cond):
        return jnp.where(cond, 1.0, 0.0).astype(BF16)

    wide_v[...] = jnp.full_like(wide_v, -1.0)
    col_v[...] = jnp.zeros_like(col_v)
    slot_v[...] = jnp.zeros_like(slot_v)
    with jax.named_scope("wait_ids"):
        l_ids.wait()
    wide_v[:, 0:64] = ids_v[...].astype(F32)
    ids = wide_v[...]
    first_id = (seq * 128).astype(F32)
    local = (ids >= first_id) & (ids < first_id + 128.0)
    block = ids - first_id
    hit = where_true(local)
    before = where_true(iota((16, 16), 1) < iota((16, 16), 0))
    counts = dot(jnp.ones((256, 16), BF16), hit)
    earlier = where_true(iota((128, 128), 0) < iota((128, 128), 1))
    rank = dot(counts[0:16].astype(BF16), earlier) + dot(before, hit)
    rank = jnp.where(local, rank, -1.0).astype(jnp.int32)
    high, low = rank >> 4, rank & 15
    digit = iota((16, 128), 0)
    token_at = iota((16, 128), 1).astype(F32)
    blocks, tokens, lows = [], [], []
    for s in range(16):
        same = high[s : s + 1, :] == digit
        blocks.append(jnp.where(same, block[s : s + 1, :], 0.0))
        tokens.append(jnp.where(same, token_at, 0.0))
        lows.append(jnp.where(low[s : s + 1, :] == digit, 1.0, 0.0))
    chosen = [jnp.concatenate(x, axis=1).astype(BF16) for x in (blocks, tokens, lows)]
    slots = dot_nt(chosen[2], jnp.concatenate(chosen[0:2], axis=0)).astype(jnp.int32)
    slot_v[:, 0:32] = slots & jnp.where(iota((16, 32), 1) < 16, 127, 63)
    to_smem = pltpu.make_async_copy(slot_v, slot_s, slot_sem)
    to_smem.start()
    cnt_v[...] = counts[0:8]
    counts = counts.astype(BF16)
    base = dot_nt(where_true(iota((64, 128), 1) < iota((64, 128), 0)), counts)
    count = dot_nt(where_true(iota((64, 128), 1) == iota((64, 128), 0)), counts)
    at = iota((64, 256), 1).astype(F32)
    tmap = jnp.where((at >= base) & (at < base + count), 1.0, 0.0)
    slot_token = jnp.sum(tmap * (iota((64, 256), 0) + 1).astype(F32), axis=0, keepdims=True)
    seg_v[...] = jnp.broadcast_to(slot_token, (8, 256))
    tmap_v[0] = tmap.astype(BF16)
    tmap_v[1] = where_true((at == base) & (count > 0.0))
    tmap_v[2] = where_true(count > 0.0)

    with jax.named_scope("wait_q"):
        wait_for(small_v, in_sem.at[2])
    wide = small_v[0].astype(F32)
    q3[...] = wide.reshape(64, 8, 128)
    q32[0:512, :] = wide
    for h in range(8):
        qh_v[h * 64 : h * 64 + 64, :] = q32[pl.ds(h, 64, stride=8), :].astype(BF16)
    rs_v[...] = dot_nt(qh_v[...], small_v[1])
    for h in range(8):
        s = rs_v[h * 64 : h * 64 + 64, :] * scale
        m = jnp.max(s, axis=1, keepdims=True)
        p = jnp.exp(s - m)
        rp_v[h * 64 : h * 64 + 64, :] = p.astype(BF16)
        col_v[0:64, h : h + 1] = m
        col_v[0:64, 8 + h : 9 + h] = jnp.sum(p, axis=1, keepdims=True)
    summed_v[...] = dot(rp_v[...], small_v[2])
    row_v[...] = col_v[...].T[0:16, :]

    lane = iota((8, 128), 1)
    empty = jnp.zeros((8, 128), F32)

    def beside(a, b):
        return jnp.concatenate([a, b], axis=1)

    def four(a, b, c, d):
        rows = [beside(a, empty), beside(empty, b), beside(c, empty), beside(empty, d)]
        return jnp.concatenate(rows, axis=0).astype(BF16)

    def apart(r):
        return r[0:8, 0:128], r[8:16, 0:128], r[16:24, 128:256], r[24:32, 128:256]

    with jax.named_scope("wait_smem"):
        l_cnt.wait()
        to_smem.wait()
    with jax.named_scope("wait_k"):
        l_k.wait()
    tops, totals = [empty, empty], [empty, empty]
    for j in range(0, CAP, 4):
        own = range(4)
        half = j // 128
        blk = [slot_s[j % 16 + i, j // 16] for i in own]
        query = [q3[slot_s[j % 16 + i, 16 + j // 16]] for i in own]
        tile = [k_v[blk[i]] for i in own]
        tile = jnp.concatenate([beside(tile[0], tile[1]), beside(tile[2], tile[3])], axis=0)
        found = apart(dot_nt(four(*query), tile))
        ps = []
        for i in own:
            here = lane == (j + i) % 128
            s = jnp.where(lane < cnt_s[blk[i]], found[i] * scale, FLOOR)
            m = jnp.max(s, axis=1, keepdims=True)
            p = jnp.exp(s - m)
            tops[half] = jnp.where(here, m, tops[half])
            totals[half] = jnp.where(here, jnp.sum(p, axis=1, keepdims=True), totals[half])
            ps.append(p)
        weight_v[j // 4] = four(*ps)
    with jax.named_scope("wait_v"):
        l_v.wait()
    for j in range(0, CAP, 4):
        tile = [v_v[slot_s[j % 16 + i, j // 16]] for i in own]
        tile = jnp.concatenate([beside(tile[0], tile[2]), beside(tile[1], tile[3])], axis=0)
        found = apart(dot(weight_v[j // 4], tile))
        for i in own:
            acc_v[pl.ds(j + i, 8, stride=STRIDE), :] = found[i]

    top, total = beside(*tops), beside(*totals)
    token = seg_v[...]
    most = top
    for back in (False, True):
        for k in (1, 2, 4, 8):
            by = 256 - k if back else k
            same = pltpu.roll(token, by, 1) == token
            most = jnp.maximum(most, jnp.where(same, pltpu.roll(most, by, 1), FLOOR))
    tmap_b, first_b = tmap_v[0], tmap_v[1]
    sum_m, sum_l = row_v[0:8, 0:64], row_v[8:16, 0:64]
    most = jnp.maximum(most, dot(sum_m.astype(BF16), tmap_b)).astype(BF16)
    shrink = jnp.exp(top - most.astype(F32))
    total = total * shrink
    total_hi = total.astype(BF16)
    total_lo = (total - total_hi.astype(F32)).astype(BF16)
    high = jnp.where(
        cnt_v[:, 0:64] > 0.0, dot_nt(most, first_b), sum_m.astype(BF16).astype(F32)
    )
    sums = dot_nt(total_hi, tmap_b) + dot_nt(total_lo, tmap_b) + sum_l * jnp.exp(sum_m - high)
    for y in range(4):
        zsend_v[y, :, 0:64] = high[2 * y : 2 * y + 2]
        zsend_v[y, :, 64:128] = sums[2 * y : 2 * y + 2]
    with jax.named_scope("barrier"):
        pl.semaphore_wait(barrier, 37)

    def remote(src, dst, send_sem, recv_sem, where):
        return pltpu.make_async_remote_copy(
            src_ref=src, dst_ref=dst, send_sem=send_sem, recv_sem=recv_sem,
            device_id=where, device_id_type=pl.DeviceIdType.MESH,
        )

    order = sorted(shifts, key=lambda d: -(min(d[0], 4 - d[0]) + min(d[1], 4 - d[1])))

    def tell(dy, dx):
        peer = seq_at(dy, dx)
        at = {"seq": peer, "kvh": keeper}
        source = zsend_v.at[peer // 4]
        remote(source, zrecv_v.at[core, dy * 4 + dx], rz_s, rz_r.at[core], at).start()

    for dy, dx in shifts:
        tell(dy, dx)

    @pl.when(core == 0)
    def _():
        tell(0, 0)

    col_m = col_v[0:64, 0:8]
    high_col = jnp.where(
        tmap_v[2][:, 0:8].astype(F32) > 0.0, dot_nt(first_b, most), col_m.astype(BF16).astype(F32)
    )
    factor = jnp.exp(col_m - high_col)
    tmap_f = tmap_b[:, 0:CAP].astype(F32)
    lane8 = iota((64, 8), 1)
    for h in range(8):
        mine = (tmap_f * shrink[h : h + 1, 0:CAP]).astype(BF16)
        a = dot(mine, acc_v[h * STRIDE : h * STRIDE + CAP, :].astype(BF16))
        keep = jnp.sum(jnp.where(lane8 == h, factor, 0.0), axis=1, keepdims=True)
        a = (a + summed_v[h * 64 : h * 64 + 64, :] * keep).astype(BF16)
        for t in range(4):
            send_v[(h // 2) * 4 + t, h % 2] = a[t * 16 : t * 16 + 16]

    def give(dy, dx):
        d = dy * 4 + dx
        peer = seq_at(dy, dx)
        at = {"seq": peer, "kvh": keeper}
        remote(send_v.at[peer], recv_v.at[core, d], rs_s, rs_r.at[core], at).start()

    for c in range(4):
        for dy in (2, 1, 3, 0):

            @pl.when((core == 0) | (sx != c) | (dy != 0))
            def _():
                give(dy, lax.rem(c - sx + 4, 4))

    def combined(group):
        heads = []
        for e in range(2):
            z = zrecv_v[group, :, e, :]
            f = jnp.exp(z - jnp.max(z, axis=0, keepdims=True))
            f = jnp.where(iota((16, 128), 1) < 64, f, 0.0)
            whole = jnp.sum(f * pltpu.roll(z, 64, 1), axis=0, keepdims=True)
            g = jnp.where(iota((16, 128), 1) < 64, f / whole, 0.0)
            g_hi = g.astype(BF16)
            g_lo = (g - g_hi.astype(F32)).astype(BF16)
            share = dot_nt(pick, g_hi) + dot_nt(pick, g_lo)
            found = jnp.zeros((16, 128), F32)
            for d in range(16):
                part = jnp.where(iota((16, 16), 1) == d, share, 0.0)
                found = found + recv_v[group, d, e].astype(F32) * jnp.sum(
                    part, axis=1, keepdims=True
                )
            piece_v[group, e] = found.astype(BF16)

    pick = where_true(iota((16, 128), 1) == iota((16, 128), 0) + 16 * sx)

    hand = remote(w_v.at[1], w_v.at[0], w_s, w_r, {"kvh": keeper})
    l_w.wait()

    @pl.when(core == 0)
    def _():
        hand.start()

    @pl.when(core == 1)
    def _():
        def place(group, o):
            return att_v.at[
                group, pl.ds(2 * (o // 4), 2), pl.ds(pl.multiple_of(16 * (o % 4), 16), 16), :
            ]

        def spread(group):
            combined(group)
            for dy, dx in order:
                at = {"seq": seq_at(dy, dx)}
                remote(
                    piece_v.at[group], place(group, seq), ag_s, ag_r.at[sx], at
                ).start()
            place(group, seq)[...] = piece_v[group]

        recv_v[1, 0] = send_v[seq]
        zrecv_v[1, 0] = zsend_v[sy]
        with jax.named_scope("rs_recv1"):
            wait_for(zrecv_v.at[1, pl.ds(1, 15)], rz_r.at[1])
            wait_for(recv_v.at[1, pl.ds(1, 15)], rs_r.at[1])
        spread(1)
        with jax.named_scope("rs_recv0"):
            wait_for(zrecv_v.at[0], rz_r.at[0])
            wait_for(recv_v.at[0], rs_r.at[0])
        spread(0)
        hand.wait_recv()

        for c in range(4):
            tokens = pl.ds(16 * c, 16)
            with jax.named_scope(f"ag_recv{c}"):

                @pl.when(sx == c)
                def _():
                    wait_for(att_v.at[:, pl.ds(0, 6), tokens], ag_r.at[c])

                @pl.when(sx != c)
                def _():
                    wait_for(att_v.at[:, :, tokens], ag_r.at[c])

            terms = None
            for g in range(2):
                rows = [att_v[g, h, 16 * c : 16 * c + 16, :] for h in range(8)]
                term = dot(jnp.concatenate(rows, axis=1), w_v[g])
                terms = term if terms is None else terms + term
            for i in range(2):
                peer = 2 * c + i
                psend_v[peer] = terms[i * 8 : i * 8 + 8].astype(BF16)

                @pl.when(kvh != peer)
                def _():
                    remote(
                        psend_v.at[peer], precv_v.at[kvh // 2], pj_s, pj_r, {"kvh": peer}
                    ).start()

        precv_v[kvh // 2] = psend_v[kvh]
        wait_for(zrecv_v.at[1, pl.ds(1, 15)], rz_s)
        wait_for(recv_v.at[1, pl.ds(1, 15)], rs_s)
        wait_for(recv_v.at[:, pl.ds(1, 15)], ag_s)
        wait_for(precv_v.at[pl.ds(0, 3)], pj_r)
        wait_for(psend_v.at[pl.ds(1, 7)], pj_s)

    @pl.when(core == 0)
    def _():
        wait_for(zrecv_v.at[0], rz_s)
        wait_for(recv_v.at[0], rs_s)
        hand.wait_send()
        with jax.named_scope("pj_recv"):
            wait_for(precv_v, pj_r)

    result = precv_v[0].astype(F32)
    for z in range(1, 4):
        result = result + precv_v[z].astype(F32)
    out_ref[...] = result.astype(BF16)


def on_device(queries, keys, values, rep_keys, rep_values, block_ids, block_counts, out_weight):
    vmem, smem, dma = pltpu.VMEM, pltpu.SMEM, pltpu.SemaphoreType.DMA
    any_spec = pl.BlockSpec(memory_space=pltpu.HBM)
    return pl.pallas_call(
        kernel,
        out_shape=jax.ShapeDtypeStruct((8, 512), BF16),
        in_specs=[any_spec] * 8,
        out_specs=pl.BlockSpec(memory_space=pltpu.VMEM),
        scratch_shapes=[
            vmem((3, 512, 128), BF16), vmem((128, 128, 128), BF16), vmem((128, 128, 128), BF16),
            vmem((16, 64), jnp.int32),
            vmem((2, 1024, 512), BF16), smem((128,), jnp.int32), vmem((16, 128), jnp.int32),
            smem((16, 128), jnp.int32),
            vmem((16, 128), F32), vmem((64, 8, 128), F32), vmem((520, 128), F32),
            vmem((512, 128), BF16), vmem((512, 512), F32), vmem((512, 512), BF16), vmem((CAP // 4, 32, 256), BF16),
            vmem((9 * STRIDE, 128), F32), vmem((512, 128), F32), vmem((8, 256), F32),
            vmem((3, 64, 256), BF16), vmem((128, 128), F32), vmem((16, 128), F32),
            vmem((8, 128), F32),
            vmem((16, 2, 16, 128), BF16), vmem((2, 16, 2, 16, 128), BF16),
            vmem((4, 2, 128), F32), vmem((2, 16, 2, 128), F32), vmem((2, 2, 16, 128), BF16),
            vmem((2, 8, 64, 128), BF16), vmem((8, 8, 512), BF16), vmem((4, 8, 512), BF16),
            dma((6,)), dma, dma, dma((2,)), dma, dma((2,)), dma, dma((4,)), dma, dma, dma, dma,
        ],
        compiler_params=pltpu.CompilerParams(collective_id=0, has_side_effects=True, vmem_limit_bytes=24 * 1024 * 1024),
        name="decode",
    )(*[pltpu.with_memory_space_constraint(x, pltpu.HBM) for x in (
        queries.reshape(-1, queries.shape[2]),
        keys.reshape(keys.shape[0], keys.shape[2], keys.shape[3]),
        values.reshape(values.shape[0], values.shape[2], values.shape[3]),
        rep_keys.reshape(-1, rep_keys.shape[3]),
        rep_values.reshape(-1, rep_values.shape[3]),
        jnp.transpose(block_ids, (1, 2, 0)).reshape(block_ids.shape[2], block_ids.shape[0]),
        block_counts,
        out_weight,
    )])


def solution(mesh):
    in_specs = (
        P(None, "kvh", None),
        P("seq", "kvh", None, None),
        P("seq", "kvh", None, None),
        P("seq", "kvh", None, None),
        P("seq", "kvh", None, None),
        P(None, "kvh", None),
        P("seq"),
        P("kvh", "seq"),
    )
    return jax.shard_map(
        on_device, mesh=mesh, in_specs=in_specs, out_specs=P("kvh", "seq"), check_vma=False
    )
```

```python
import functools
import math

import jax
import jax.numpy as jnp
from jax import lax
from jax.experimental import pallas as pl
from jax.experimental.pallas import tpu as pltpu
from jax.sharding import PartitionSpec as P

CAP = 192
STRIDE = 196
FLOOR = -1e30
F32 = jnp.float32
BF16 = jnp.bfloat16
NT = (((1,), (1,)), ((), ()))


def dot(a, b):
    return jnp.dot(a, b, preferred_element_type=F32)


def dot_nt(a, b):
    return lax.dot_general(a, b, NT, preferred_element_type=F32)


def iota(shape, dim):
    return lax.broadcasted_iota(jnp.int32, shape, dim)


def kernel(
    q_hbm, k_hbm, v_hbm, rk_hbm, rv_hbm, ids_hbm, cnt_hbm, w_hbm,
    out_ref,
    small_v, k_v, v_v, ids_v, w_v, cnt_s, slot_v, slot_s,
    wide_v, q3, q32, qh_v, rs_v, rp_v, weight_v, acc_v, summed_v, seg_v,
    tmap_v, col_v, row_v, cnt_v, send_v, recv_v, zsend_v, zrecv_v, piece_v, att_v, psend_v, precv_v,
    in_sem, slot_sem, rs_s, rs_r, rz_s, rz_r, ag_s, ag_r, pj_s, pj_r, w_s, w_r,
):
    seq = lax.axis_index("seq")
    kvh = lax.axis_index("kvh")
    sy, sx = seq // 4, seq % 4
    core = lax.rem(kvh, 2)
    other = kvh + 1 - 2 * core
    keeper = kvh + 1 - core
    scale = 1.0 / math.sqrt(128)

    def seq_at(dy, dx):
        return lax.rem(sy + dy + 4, 4) * 4 + lax.rem(sx + dx + 4, 4)

    shifts = [(dy, dx) for dy in range(4) for dx in range(4) if dy or dx]

    barrier = pltpu.get_barrier_semaphore()
    loads = [
        pltpu.make_async_copy(src, dst, in_sem.at[i])
        for src, dst, i in [
            (ids_hbm, ids_v, 0), (cnt_hbm, cnt_s, 1), (q_hbm, small_v.at[0], 2),
            (rk_hbm, small_v.at[1], 2), (rv_hbm, small_v.at[2], 2), (k_hbm, k_v, 3),
            (v_hbm, v_v, 4), (w_hbm, w_v.at[1], 5),
        ]
    ]
    for load in loads:
        load.start()
    l_ids, l_cnt, _, _, _, l_k, l_v, l_w = loads

    def wait_for(like, sem):
        pltpu.make_async_copy(like, like, sem).wait()

    for dy, dx in shifts:
        pl.semaphore_signal(
            barrier, inc=1, device_id={"seq": seq_at(dy, dx)}, device_id_type=pl.DeviceIdType.MESH
        )
        pl.semaphore_signal(
            barrier,
            inc=1,
            device_id={"seq": seq_at(dy, dx), "kvh": other},
            device_id_type=pl.DeviceIdType.MESH,
        )
    for e in range(1, 8):
        pl.semaphore_signal(
            barrier, inc=1, device_id={"kvh": lax.rem(kvh + e, 8)}, device_id_type=pl.DeviceIdType.MESH
        )

    def where_true(cond):
        return jnp.where(cond, 1.0, 0.0).astype(BF16)

    wide_v[...] = jnp.full_like(wide_v, -1.0)
    col_v[...] = jnp.zeros_like(col_v)
    slot_v[...] = jnp.zeros_like(slot_v)
    with jax.named_scope("wait_ids"):
        l_ids.wait()
    wide_v[:, 0:64] = ids_v[...].astype(F32)
    ids = wide_v[...]
    first_id = (seq * 128).astype(F32)
    local = (ids >= first_id) & (ids < first_id + 128.0)
    block = ids - first_id
    hit = where_true(local)
    before = where_true(iota((16, 16), 1) < iota((16, 16), 0))
    counts = dot(jnp.ones((256, 16), BF16), hit)
    earlier = where_true(iota((128, 128), 0) < iota((128, 128), 1))
    rank = dot(counts[0:16].astype(BF16), earlier) + dot(before, hit)
    rank = jnp.where(local, rank, -1.0).astype(jnp.int32)
    high, low = rank >> 4, rank & 15
    digit = iota((16, 128), 0)
    token_at = iota((16, 128), 1).astype(F32)
    blocks, tokens, lows = [], [], []
    for s in range(16):
        same = high[s : s + 1, :] == digit
        blocks.append(jnp.where(same, block[s : s + 1, :], 0.0))
        tokens.append(jnp.where(same, token_at, 0.0))
        lows.append(jnp.where(low[s : s + 1, :] == digit, 1.0, 0.0))
    chosen = [jnp.concatenate(x, axis=1).astype(BF16) for x in (blocks, tokens, lows)]
    slots = dot_nt(chosen[2], jnp.concatenate(chosen[0:2], axis=0)).astype(jnp.int32)
    slot_v[:, 0:32] = slots & jnp.where(iota((16, 32), 1) < 16, 127, 63)
    to_smem = pltpu.make_async_copy(slot_v, slot_s, slot_sem)
    to_smem.start()
    cnt_v[...] = counts[0:8]
    counts = counts.astype(BF16)
    base = dot_nt(where_true(iota((64, 128), 1) < iota((64, 128), 0)), counts)
    count = dot_nt(where_true(iota((64, 128), 1) == iota((64, 128), 0)), counts)
    at = iota((64, 256), 1).astype(F32)
    tmap = jnp.where((at >= base) & (at < base + count), 1.0, 0.0)
    slot_token = jnp.sum(tmap * (iota((64, 256), 0) + 1).astype(F32), axis=0, keepdims=True)
    seg_v[...] = jnp.broadcast_to(slot_token, (8, 256))
    tmap_v[0] = tmap.astype(BF16)
    tmap_v[1] = where_true((at == base) & (count > 0.0))
    tmap_v[2] = where_true(count > 0.0)

    with jax.named_scope("wait_q"):
        wait_for(small_v, in_sem.at[2])
    wide = small_v[0].astype(F32)
    q3[...] = wide.reshape(64, 8, 128)
    q32[0:512, :] = wide
    for h in range(8):
        qh_v[h * 64 : h * 64 + 64, :] = q32[pl.ds(h, 64, stride=8), :].astype(BF16)
    rs_v[...] = dot_nt(qh_v[...], small_v[1])
    for h in range(8):
        s = rs_v[h * 64 : h * 64 + 64, :] * scale
        m = jnp.max(s, axis=1, keepdims=True)
        p = jnp.exp(s - m)
        rp_v[h * 64 : h * 64 + 64, :] = p.astype(BF16)
        col_v[0:64, h : h + 1] = m
        col_v[0:64, 8 + h : 9 + h] = jnp.sum(p, axis=1, keepdims=True)
    summed_v[...] = dot(rp_v[...], small_v[2])
    row_v[...] = col_v[...].T[0:16, :]

    lane = iota((8, 128), 1)
    empty = jnp.zeros((8, 128), F32)

    def beside(a, b):
        return jnp.concatenate([a, b], axis=1)

    def four(a, b, c, d):
        rows = [beside(a, empty), beside(empty, b), beside(c, empty), beside(empty, d)]
        return jnp.concatenate(rows, axis=0).astype(BF16)

    def apart(r):
        return r[0:8, 0:128], r[8:16, 0:128], r[16:24, 128:256], r[24:32, 128:256]

    with jax.named_scope("wait_smem"):
        l_cnt.wait()
        to_smem.wait()
    with jax.named_scope("wait_k"):
        l_k.wait()
    tops, totals = [empty, empty], [empty, empty]
    for j in range(0, CAP, 4):
        own = range(4)
        half = j // 128
        blk = [slot_s[j % 16 + i, j // 16] for i in own]
        query = [q3[slot_s[j % 16 + i, 16 + j // 16]] for i in own]
        tile = [k_v[blk[i]] for i in own]
        tile = jnp.concatenate([beside(tile[0], tile[1]), beside(tile[2], tile[3])], axis=0)
        found = apart(dot_nt(four(*query), tile))
        ps = []
        for i in own:
            here = lane == (j + i) % 128
            s = jnp.where(lane < cnt_s[blk[i]], found[i] * scale, FLOOR)
            m = jnp.max(s, axis=1, keepdims=True)
            p = jnp.exp(s - m)
            tops[half] = jnp.where(here, m, tops[half])
            totals[half] = jnp.where(here, jnp.sum(p, axis=1, keepdims=True), totals[half])
            ps.append(p)
        weight_v[j // 4] = four(*ps)
    with jax.named_scope("wait_v"):
        l_v.wait()
    for j in range(0, CAP, 4):
        tile = [v_v[slot_s[j % 16 + i, j // 16]] for i in own]
        tile = jnp.concatenate([beside(tile[0], tile[2]), beside(tile[1], tile[3])], axis=0)
        found = apart(dot(weight_v[j // 4], tile))
        for i in own:
            acc_v[pl.ds(j + i, 8, stride=STRIDE), :] = found[i]

    top, total = beside(*tops), beside(*totals)
    token = seg_v[...]
    most = top
    for back in (False, True):
        for k in (1, 2, 4, 8):
            by = 256 - k if back else k
            same = pltpu.roll(token, by, 1) == token
            most = jnp.maximum(most, jnp.where(same, pltpu.roll(most, by, 1), FLOOR))
    tmap_b, first_b = tmap_v[0], tmap_v[1]
    sum_m, sum_l = row_v[0:8, 0:64], row_v[8:16, 0:64]
    most = jnp.maximum(most, dot(sum_m.astype(BF16), tmap_b)).astype(BF16)
    shrink = jnp.exp(top - most.astype(F32))
    total = total * shrink
    total_hi = total.astype(BF16)
    total_lo = (total - total_hi.astype(F32)).astype(BF16)
    high = jnp.where(
        cnt_v[:, 0:64] > 0.0, dot_nt(most, first_b), sum_m.astype(BF16).astype(F32)
    )
    sums = dot_nt(total_hi, tmap_b) + dot_nt(total_lo, tmap_b) + sum_l * jnp.exp(sum_m - high)
    for y in range(4):
        zsend_v[y, :, 0:64] = high[2 * y : 2 * y + 2]
        zsend_v[y, :, 64:128] = sums[2 * y : 2 * y + 2]
    with jax.named_scope("barrier"):
        pl.semaphore_wait(barrier, 37)

    def remote(src, dst, send_sem, recv_sem, where):
        return pltpu.make_async_remote_copy(
            src_ref=src, dst_ref=dst, send_sem=send_sem, recv_sem=recv_sem,
            device_id=where, device_id_type=pl.DeviceIdType.MESH,
        )

    order = sorted(shifts, key=lambda d: -(min(d[0], 4 - d[0]) + min(d[1], 4 - d[1])))

    def tell(dy, dx):
        peer = seq_at(dy, dx)
        at = {"seq": peer, "kvh": keeper}
        source = zsend_v.at[peer // 4]
        remote(source, zrecv_v.at[core, dy * 4 + dx], rz_s, rz_r.at[core], at).start()

    for dy, dx in shifts:
        tell(dy, dx)

    @pl.when(core == 0)
    def _():
        tell(0, 0)

    col_m = col_v[0:64, 0:8]
    high_col = jnp.where(
        tmap_v[2][:, 0:8].astype(F32) > 0.0, dot_nt(first_b, most), col_m.astype(BF16).astype(F32)
    )
    factor = jnp.exp(col_m - high_col)
    tmap_f = tmap_b[:, 0:CAP].astype(F32)
    lane8 = iota((64, 8), 1)
    for h in range(8):
        mine = (tmap_f * shrink[h : h + 1, 0:CAP]).astype(BF16)
        a = dot(mine, acc_v[h * STRIDE : h * STRIDE + CAP, :].astype(BF16))
        keep = jnp.sum(jnp.where(lane8 == h, factor, 0.0), axis=1, keepdims=True)
        a = (a + summed_v[h * 64 : h * 64 + 64, :] * keep).astype(BF16)
        for t in range(4):
            send_v[(h // 2) * 4 + t, h % 2] = a[t * 16 : t * 16 + 16]

    def give(dy, dx):
        d = dy * 4 + dx
        peer = seq_at(dy, dx)
        at = {"seq": peer, "kvh": keeper}
        remote(send_v.at[peer], recv_v.at[core, d], rs_s, rs_r.at[core], at).start()

    for c in range(4):
        for dy in (2, 1, 3, 0):

            @pl.when((core == 0) | (sx != c) | (dy != 0))
            def _():
                give(dy, lax.rem(c - sx + 4, 4))

    def combined(group):
        heads = []
        for e in range(2):
            z = zrecv_v[group, :, e, :]
            f = jnp.exp(z - jnp.max(z, axis=0, keepdims=True))
            f = jnp.where(iota((16, 128), 1) < 64, f, 0.0)
            whole = jnp.sum(f * pltpu.roll(z, 64, 1), axis=0, keepdims=True)
            g = jnp.where(iota((16, 128), 1) < 64, f / whole, 0.0)
            g_hi = g.astype(BF16)
            g_lo = (g - g_hi.astype(F32)).astype(BF16)
            share = dot_nt(pick, g_hi) + dot_nt(pick, g_lo)
            found = jnp.zeros((16, 128), F32)
            for d in range(16):
                part = jnp.where(iota((16, 16), 1) == d, share, 0.0)
                found = found + recv_v[group, d, e].astype(F32) * jnp.sum(
                    part, axis=1, keepdims=True
                )
            piece_v[group, e] = found.astype(BF16)

    pick = where_true(iota((16, 128), 1) == iota((16, 128), 0) + 16 * sx)

    hand = remote(w_v.at[1], w_v.at[0], w_s, w_r, {"kvh": keeper})
    l_w.wait()

    @pl.when(core == 0)
    def _():
        hand.start()

    @pl.when(core == 1)
    def _():
        def place(group, o):
            return att_v.at[
                group, pl.ds(2 * (o // 4), 2), pl.ds(pl.multiple_of(16 * (o % 4), 16), 16), :
            ]

        def spread(group):
            combined(group)
            for dy, dx in order:
                at = {"seq": seq_at(dy, dx)}
                remote(
                    piece_v.at[group], place(group, seq), ag_s, ag_r.at[group, sx], at
                ).start()
            place(group, seq)[...] = piece_v[group]

        recv_v[1, 0] = send_v[seq]
        zrecv_v[1, 0] = zsend_v[sy]
        with jax.named_scope("rs_recv1"):
            wait_for(zrecv_v.at[1, pl.ds(1, 15)], rz_r.at[1])
            wait_for(recv_v.at[1, pl.ds(1, 15)], rs_r.at[1])
        spread(1)
        with jax.named_scope("rs_recv0"):
            wait_for(zrecv_v.at[0], rz_r.at[0])
            wait_for(recv_v.at[0], rs_r.at[0])
        spread(0)
        hand.wait_recv()

        for c in range(4):
            tokens = pl.ds(16 * c, 16)
            terms = None
            for g in (1, 0):

                @pl.when(sx == c)
                def _():
                    wait_for(att_v.at[g, pl.ds(0, 6), tokens], ag_r.at[g, c])

                @pl.when(sx != c)
                def _():
                    wait_for(att_v.at[g, :, tokens], ag_r.at[g, c])

                rows = [att_v[g, h, 16 * c : 16 * c + 16, :] for h in range(8)]
                term = dot(jnp.concatenate(rows, axis=1), w_v[g])
                terms = term if terms is None else terms + term
            for i in range(2):
                peer = 2 * c + i
                psend_v[peer] = terms[i * 8 : i * 8 + 8].astype(BF16)

                @pl.when(kvh != peer)
                def _():
                    remote(
                        psend_v.at[peer], precv_v.at[kvh // 2], pj_s, pj_r, {"kvh": peer}
                    ).start()

        precv_v[kvh // 2] = psend_v[kvh]
        wait_for(zrecv_v.at[1, pl.ds(1, 15)], rz_s)
        wait_for(recv_v.at[1, pl.ds(1, 15)], rs_s)
        wait_for(recv_v.at[:, pl.ds(1, 15)], ag_s)
        wait_for(precv_v.at[pl.ds(0, 3)], pj_r)
        wait_for(psend_v.at[pl.ds(1, 7)], pj_s)

    @pl.when(core == 0)
    def _():
        wait_for(zrecv_v.at[0], rz_s)
        wait_for(recv_v.at[0], rs_s)
        hand.wait_send()
        with jax.named_scope("pj_recv"):
            wait_for(precv_v, pj_r)

    result = precv_v[0].astype(F32)
    for z in range(1, 4):
        result = result + precv_v[z].astype(F32)
    out_ref[...] = result.astype(BF16)


def on_device(queries, keys, values, rep_keys, rep_values, block_ids, block_counts, out_weight):
    vmem, smem, dma = pltpu.VMEM, pltpu.SMEM, pltpu.SemaphoreType.DMA
    any_spec = pl.BlockSpec(memory_space=pltpu.HBM)
    return pl.pallas_call(
        kernel,
        out_shape=jax.ShapeDtypeStruct((8, 512), BF16),
        in_specs=[any_spec] * 8,
        out_specs=pl.BlockSpec(memory_space=pltpu.VMEM),
        scratch_shapes=[
            vmem((3, 512, 128), BF16), vmem((128, 128, 128), BF16), vmem((128, 128, 128), BF16),
            vmem((16, 64), jnp.int32),
            vmem((2, 1024, 512), BF16), smem((128,), jnp.int32), vmem((16, 128), jnp.int32),
            smem((16, 128), jnp.int32),
            vmem((16, 128), F32), vmem((64, 8, 128), F32), vmem((520, 128), F32),
            vmem((512, 128), BF16), vmem((512, 512), F32), vmem((512, 512), BF16), vmem((CAP // 4, 32, 256), BF16),
            vmem((9 * STRIDE, 128), F32), vmem((512, 128), F32), vmem((8, 256), F32),
            vmem((3, 64, 256), BF16), vmem((128, 128), F32), vmem((16, 128), F32),
            vmem((8, 128), F32),
            vmem((16, 2, 16, 128), BF16), vmem((2, 16, 2, 16, 128), BF16),
            vmem((4, 2, 128), F32), vmem((2, 16, 2, 128), F32), vmem((2, 2, 16, 128), BF16),
            vmem((2, 8, 64, 128), BF16), vmem((8, 8, 512), BF16), vmem((4, 8, 512), BF16),
            dma((6,)), dma, dma, dma((2,)), dma, dma((2,)), dma, dma((2, 4)), dma, dma, dma, dma,
        ],
        compiler_params=pltpu.CompilerParams(collective_id=0, has_side_effects=True, vmem_limit_bytes=24 * 1024 * 1024),
        name="decode",
    )(*[pltpu.with_memory_space_constraint(x, pltpu.HBM) for x in (
        queries.reshape(-1, queries.shape[2]),
        keys.reshape(keys.shape[0], keys.shape[2], keys.shape[3]),
        values.reshape(values.shape[0], values.shape[2], values.shape[3]),
        rep_keys.reshape(-1, rep_keys.shape[3]),
        rep_values.reshape(-1, rep_values.shape[3]),
        jnp.transpose(block_ids, (1, 2, 0)).reshape(block_ids.shape[2], block_ids.shape[0]),
        block_counts,
        out_weight,
    )])


def solution(mesh):
    in_specs = (
        P(None, "kvh", None),
        P("seq", "kvh", None, None),
        P("seq", "kvh", None, None),
        P("seq", "kvh", None, None),
        P("seq", "kvh", None, None),
        P(None, "kvh", None),
        P("seq"),
        P("kvh", "seq"),
    )
    return jax.shard_map(
        on_device, mesh=mesh, in_specs=in_specs, out_specs=P("kvh", "seq"), check_vma=False
    )
```
